512 devices in a mesh: gx: 4 (over z_hi), gy: 8 (over y, core), gz: 16 (over x, z_lo).
Axes of the slice: x: 4, y: 4, z: 16 (z_hi: 4, z_lo: 4; z = z_hi * 4 + z_lo), core: 2. Of those that a mesh axis runs over, the one named last changes fastest.
Arguments:
- right_side: float32 [4, 8, 16, 6, 1024], P('gx', 'gy', 'gz'), may hold values from -18 to 18
- grain_diag: float32 [4, 8, 16, 6, 1024], P('gx', 'gy', 'gz'), may hold values from 0.05 to 0.5
- stiffness: float32 [4, 4], replicated, may hold values from 0.3 to 3
- contact_own: int32 [4, 8, 16, 3072], P('gx', 'gy', 'gz'), may hold values from 0 to 1023, as said below
- contact_slot: int32 [4, 8, 16, 3072], P('gx', 'gy', 'gz'), may hold values from 0 to 7679, as said below
- contact_type: int32 [4, 8, 16, 3072], P('gx', 'gy', 'gz'), may hold values from 0 to 4, as said below
- contact_normal: float32 [4, 8, 16, 3, 3072], P('gx', 'gy', 'gz'), may hold values from -1 to 1, as said below
- contact_radii: float32 [4, 8, 16, 2, 3072], P('gx', 'gy', 'gz'), may hold values from 0.4 to 1
Outputs:
- solution_field: float32 [4, 8, 16, 6, 1024], P('gx', 'gy', 'gz')
- residual: float32 [4, 8, 16, 6, 1024], P('gx', 'gy', 'gz')
The draws below stay inside these ranges and needn't reach their ends.
Inputs may be any that keep to these rules, and one draw needn't show every extreme that they name: `contact_normal`: each normal has unit length. `contact_own`: in the first 2240 slots of a block the own grain differs from the partner; in the last 832 slots the own grain is one of the block's first 256 grains. `contact_slot`: the first 2240 slots of a block hold values below 1024; the slots 3072 - 832 + k * 32 to 2240 + (k + 1) * 32 - 1, for k = 0 to 25, hold values from 1024 + k * 256 to 1024 + (k + 1) * 256 - 1. `contact_type`: the value 4 marks an empty slot.
All inputs are finite; a program needn't handle non-finite values.
Results may differ from the reference program's by a relative error of at most 0.00018.
Values sent between devices are 32-bit elements; how exact they have to be, the bound alone decides.
A program may use at most 64 MiB of HBM per device.

```python
import math
import jax
import jax.numpy as jnp

GRAINS = 1024
RIM = 256
CONTACTS = 3072
GROUP = 32
REMOTE = 832
TYPES = 4
ITERS = 4
BX = 4
BY = 8
BZ = 16


def contact_tables(key):
    base = jax.random.fold_in(key, 7301)
    keys = jax.random.split(base, 6)
    lead = (BX, BY, BZ)
    local_count = CONTACTS - REMOTE
    own_near = jax.random.randint(keys[0], lead + (local_count,), 0, GRAINS, dtype=jnp.int32)
    offset = jax.random.randint(keys[1], lead + (local_count,), 1, GRAINS, dtype=jnp.int32)
    slot_near = (own_near + offset) % GRAINS
    own_far = jax.random.randint(keys[2], lead + (REMOTE,), 0, RIM, dtype=jnp.int32)
    neighbour = jnp.broadcast_to(jnp.arange(REMOTE, dtype=jnp.int32) // GROUP, lead + (REMOTE,))
    ghost = jax.random.randint(keys[4], lead + (REMOTE,), 0, RIM, dtype=jnp.int32)
    slot_far = GRAINS + neighbour * RIM + ghost
    ctype = jax.random.randint(keys[5], lead + (CONTACTS,), 0, TYPES + 1, dtype=jnp.int32)
    owners = jnp.concatenate([own_near, own_far], axis=-1)
    slots = jnp.concatenate([slot_near, slot_far], axis=-1)
    return (owners, slots, ctype)


def draw_contact_own(key, part):
    return contact_tables(key)[0]


def draw_contact_slot(key, part):
    return contact_tables(key)[1]


def draw_contact_type(key, part):
    return contact_tables(key)[2]


def draw_contact_normal(key, part):
    inner = jax.random.fold_in(key, 4409)
    vectors = jax.random.normal(inner, (BX, BY, BZ, 3, CONTACTS), jnp.float32)
    length = jnp.sqrt(jnp.sum(vectors * vectors, axis=3, keepdims=True) + 1e-12)
    return vectors / length


def draw_right_side(key, part):
    inner = jax.random.fold_in(key, 1187)
    index = (jnp.arange(BX)[:, None, None] * BY + jnp.arange(BY)[None, :, None]) * BZ + jnp.arange(BZ)[None, None, :]
    ramp = index.astype(jnp.float32) / max(BX * BY * BZ - 1, 1)
    scale = (1.0 + 2.0 * ramp)[:, :, :, None, None]
    values = jnp.clip(jax.random.normal(inner, (BX, BY, BZ, 6, GRAINS), jnp.float32), -6.0, 6.0) * scale
    return values


def level_of(stream_key, extent, shards, low, top_value):
    def one(position, shards_of):
        heights = jax.random.uniform(jax.random.fold_in(jax.random.fold_in(stream_key, 6), position), (shards_of,), jnp.float32, low / len(shards), top_value / len(shards))
        return jnp.repeat(jnp.exp(heights), extent[position] // shards_of).reshape((-1,) + (1,) * (len(extent) - position - 1))

    loudness = one(*shards[0])
    for cut in shards[1:]:
        loudness = loudness * one(*cut)
    return loudness


def setup_inputs(seed: int = 0) -> dict:
    seeds = jax.random.split(jax.random.key(seed), 9)
    return {
        "right_side": draw_right_side(jax.random.fold_in(seeds[8], 71), 0),
        "grain_diag": jnp.clip(jnp.exp(math.log(0.5) - 2.3025851 * jax.random.uniform(seeds[1], (BX, BY, BZ, 6, GRAINS), jnp.float32) ** level_of(seeds[1], (BX, BY, BZ, 6, GRAINS), ((0, 4), (1, 8), (2, 16)), -0.2, 0.2)), 0.05, 0.5),
        "stiffness": jnp.clip(jnp.exp(jax.random.uniform(seeds[2], (4, TYPES), jnp.float32, math.log(0.3), math.log(3.0))), 0.3, 3.0),
        "contact_own": draw_contact_own(jax.random.fold_in(seeds[8], 71), 0),
        "contact_slot": draw_contact_slot(jax.random.fold_in(seeds[8], 71), 0),
        "contact_type": draw_contact_type(jax.random.fold_in(seeds[8], 71), 0),
        "contact_normal": draw_contact_normal(jax.random.fold_in(seeds[8], 71), 0),
        "contact_radii": jnp.clip(jnp.exp(math.log(1.0) - 0.9162907 * jax.random.uniform(seeds[7], (BX, BY, BZ, 2, CONTACTS), jnp.float32) ** level_of(seeds[7], (BX, BY, BZ, 2, CONTACTS), ((0, 4), (1, 8), (2, 16)), -0.2, 0.2)), 0.4, 1.0),
    }


def cross(left, right):
    return jnp.stack([left[1] * right[2] - left[2] * right[1],
                      left[2] * right[0] - left[0] * right[2],
                      left[0] * right[1] - left[1] * right[0]])


def lookup(stiffness, ctype):
    total = jnp.zeros((4,) + ctype.shape, stiffness.dtype)
    for which in range(stiffness.shape[1]):
        total = total + stiffness[:, which:which + 1] * (ctype == which)[None].astype(stiffness.dtype)
    return total


def contact_response(first_u, second_u, normal, radii, coeff):
    normal_k, shear_k, roll_k, twist_k = coeff[0], coeff[1], coeff[2], coeff[3]
    first_r, second_r = radii[0], radii[1]
    delta = second_u[:3] - second_r * cross(second_u[3:], normal) - first_u[:3] - first_r * cross(first_u[3:], normal)
    along = jnp.sum(normal * delta, axis=0)
    force = shear_k * delta + (normal_k - shear_k) * along * normal
    theta = second_u[3:] - first_u[3:]
    twist = jnp.sum(normal * theta, axis=0)
    moment = roll_k * theta + (twist_k - roll_k) * twist * normal
    lever = cross(normal, force)
    on_first = jnp.concatenate([force, first_r * lever + moment], axis=0)
    on_second = jnp.concatenate([-force, second_r * lever - moment], axis=0)
    return on_first, on_second


def flatten_field(array):
    return jnp.moveaxis(array, 3, 0).reshape(array.shape[3], -1)


def reference(right_side, grain_diag, stiffness, contact_own, contact_slot, contact_type, contact_normal, contact_radii):
    rhs = flatten_field(right_side)
    diag = flatten_field(grain_diag)
    normal = flatten_field(contact_normal)
    radii = flatten_field(contact_radii)
    block_x = jnp.arange(BX, dtype=jnp.int32)[:, None, None, None]
    block_y = jnp.arange(BY, dtype=jnp.int32)[None, :, None, None]
    block_z = jnp.arange(BZ, dtype=jnp.int32)[None, None, :, None]
    base = ((block_x * BY + block_y) * BZ + block_z) * GRAINS
    remote = contact_slot >= GRAINS
    rel = jnp.maximum(contact_slot - GRAINS, 0)
    kk = rel // RIM
    full = kk + (kk >= 13).astype(jnp.int32)
    off_x = full // 9 - 1
    off_y = (full // 3) % 3 - 1
    off_z = full % 3 - 1
    other = ((((block_x + off_x) % BX) * BY + (block_y + off_y) % BY) * BZ + (block_z + off_z) % BZ) * GRAINS
    first = (base + contact_own).reshape(-1).astype(jnp.int32)
    second = jnp.where(remote, other + rel % RIM, base + contact_slot).reshape(-1).astype(jnp.int32)
    coeff = lookup(stiffness, contact_type.reshape(-1))

    def operate(field):
        on_first, on_second = contact_response(field[:, first], field[:, second], normal, radii, coeff)
        forces = jnp.zeros_like(field).at[:, first].add(on_first).at[:, second].add(on_second)
        return diag * field - forces

    solution_field = jnp.zeros_like(rhs)
    residual = rhs
    direction = rhs
    norm_now = jnp.sum(residual * residual)
    for step in range(ITERS):
        image = operate(direction)
        alpha = norm_now / jnp.sum(direction * image)
        solution_field = solution_field + alpha * direction
        residual = residual - alpha * image
        norm_next = jnp.sum(residual * residual)
        direction = residual + (norm_next / norm_now) * direction
        norm_now = norm_next

    def unflatten(field):
        return jnp.moveaxis(field.reshape(6, BX, BY, BZ, GRAINS), 0, 3)

    return unflatten(solution_field), unflatten(residual)
```

```python
import functools

import jax
import jax.numpy as jnp
from jax import lax
from jax.experimental import pallas as pl
from jax.experimental.pallas import tpu as pltpu
from jax.sharding import PartitionSpec as P

F32 = jnp.float32
BF16 = jnp.bfloat16
MESH = pl.DeviceIdType.MESH
GRAINS = 1024
RIM = 256
NEAR = 2240
TYPES = 4
SIDES = 26
LOCAL_ROWS = 18
NX, NY, NZ = 4, 8, 16
ZLO = 4
PLANE = 32
LINE = 16


def offset_of(side):
    whole = side + (1 if side >= 13 else 0)
    return (whole // 9 - 1, whole // 3 % 3 - 1, whole % 3 - 1)


def cross(w, n):
    return [
        w[1] * n[2] - w[2] * n[1],
        w[2] * n[0] - w[0] * n[2],
        w[0] * n[1] - w[1] * n[0],
    ]


def response(a, b, n, ra, rb, coeff, both):
    shear, normal_less, roll, twist_less = coeff
    arm = [rb * b[3 + c] + ra * a[3 + c] for c in range(3)]
    turn = cross(arm, n)
    delta = [b[c] - a[c] - turn[c] for c in range(3)]
    along = normal_less * (n[0] * delta[0] + n[1] * delta[1] + n[2] * delta[2])
    force = [shear * delta[c] + along * n[c] for c in range(3)]
    theta = [b[3 + c] - a[3 + c] for c in range(3)]
    twist = twist_less * (n[0] * theta[0] + n[1] * theta[1] + n[2] * theta[2])
    moment = [roll * theta[c] + twist * n[c] for c in range(3)]
    lever = cross(n, force)
    first = force + [ra * lever[c] + moment[c] for c in range(3)]
    if not both:
        return first, None
    second = [-f for f in force] + [rb * lever[c] - moment[c] for c in range(3)]
    return first, second


def lanes(x, index):
    return jnp.take_along_axis(x, index, axis=1, mode="promise_in_bounds")


def splat(row):
    return jnp.broadcast_to(row, (8, 128))


def kernel(
    rhs_ref, diag_ref, stiff_ref, own_ref, slot_ref, type_ref, normal_ref, radii_ref,
    x_ref, r_ref,
    dense, idx_a, idx_b, geo, one_hot, t_local, lhs_local,
    rim_idx, rim_geo, rim_hot, t_rim, lhs_rim, field, mine,
    send_q, recv_q, send_v, recv_v, row_buf, plane_buf, line_buf,
    q_send, q_recv, v_send, v_recv, s_send, s_recv,
):
    gx, gy, gz = lax.axis_index("gx"), lax.axis_index("gy"), lax.axis_index("gz")
    wide, low = gz // ZLO, gz % ZLO

    near = []
    for side in range(SIDES):
        dx, dy, dz = offset_of(side)
        near.append(((gx + (dx + NX)) % NX, (gy + (dy + NY)) % NY, (gz + (dz + NZ)) % NZ))
    plane = []
    for j in range(1, PLANE):
        dy, dw = j // ZLO, j % ZLO
        plane.append((gx, (gy + dy) % NY, ((wide + dw) % ZLO) * ZLO + low))
    line = []
    for j in range(1, LINE):
        dx, dl = j // ZLO, j % ZLO
        line.append(((gx + dx) % NX, gy, wide * ZLO + (low + dl) % ZLO))
    plane_rank = gy * ZLO + wide
    line_rank = gx * ZLO + low

    lane = lax.broadcasted_iota(jnp.int32, (8, 128), 1)
    row = lax.broadcasted_iota(jnp.int32, (8, 128), 0)

    recv_q[0:2] = jnp.zeros((2, 2, 128), F32)
    recv_q[28:32] = jnp.zeros((4, 2, 128), F32)
    for e in range(4):
        recv_v[e, 0:2] = jnp.zeros((2, 3, 128), F32)
        recv_v[e, 28:32] = jnp.zeros((4, 3, 128), F32)

    barrier = pltpu.get_barrier_semaphore()
    for where in near + plane + line:
        pl.semaphore_signal(barrier, inc=1, device_id=where, device_id_type=MESH)

    for i in range(24):
        cut = slice(128 * i, 128 * (i + 1))
        dense[0, i : i + 1, :] = own_ref[0, 0, :, cut].astype(F32)
        dense[1, i : i + 1, :] = slot_ref[0, 0, :, cut].astype(F32)
        dense[2, i : i + 1, :] = type_ref[0, 0, :, cut].astype(F32)
        for c in range(3):
            dense[3 + c, i : i + 1, :] = normal_ref[0, 0, 0, c : c + 1, cut]
        for c in range(2):
            dense[6 + c, i : i + 1, :] = radii_ref[0, 0, 0, c : c + 1, cut]

    def coefficients(kind, valid):
        out = []
        for q in range(4):
            total = jnp.zeros_like(kind)
            for t in range(TYPES):
                total = jnp.where(kind == float(t), stiff_ref[q, t], total)
            out.append(jnp.where(valid, total, 0.0))
        return [out[1], out[0] - out[1], out[2], out[3] - out[2]]

    def segments(q, v):
        low_row = dense[q, 17 + 2 * v : 18 + 2 * v, :]
        nxt = min(18 + 2 * v, 23)
        high_row = dense[q, nxt : nxt + 1, :]
        base = jnp.where(row < 4, splat(low_row), splat(high_row))
        return lanes(base, (lane % 32) + 32 * (row % 4))

    def quarter(parts):
        out = parts[3]
        for p in (2, 1, 0):
            out = jnp.where(lane < 32 * (p + 1), parts[p], out)
        return out

    kept = []
    for v in range(4):
        seg = [segments(q, v) for q in range(8)]
        side = (row + (8 * v - 2)).astype(F32)
        slot_rim = seg[1] - (GRAINS + RIM * side)
        rows = slice(8 * v, 8 * v + 8)
        send_q[rows, 0, :] = quarter([slot_rim, seg[2], seg[6], seg[7]])
        send_q[rows, 1, :] = quarter([seg[3], seg[4], seg[5], seg[5]])
        kept.append(seg)
    for v in range(4):
        for q in range(8):
            rim_geo[q, 8 * v : 8 * v + 8, :] = kept[v][q]

    pl.semaphore_wait(barrier, SIDES + PLANE - 1 + LINE - 1)

    q_copies = []
    for side in range(SIDES):
        copy = pltpu.make_async_remote_copy(
            src_ref=send_q.at[side + 2],
            dst_ref=recv_q.at[27 - side],
            send_sem=q_send.at[side],
            recv_sem=q_recv.at[25 - side],
            device_id=near[side],
            device_id_type=MESH,
        )
        copy.start()
        q_copies.append(copy)

    for v in range(3):
        rows = slice(8 * v, 8 * v + 8)
        number = (row + 8 * v) * 128 + lane
        inside = number < NEAR
        own = dense[0, rows, :]
        slot = jnp.where(inside, dense[1, rows, :], 0.0)
        idx_a[rows, :] = own.astype(jnp.int32)
        idx_b[rows, :] = slot.astype(jnp.int32)
        dense[1, rows, :] = slot
        coeff = coefficients(dense[2, rows, :], inside)
        for q in range(4):
            geo[q, rows, :] = coeff[q]

    column = lax.broadcasted_iota(jnp.int32, (128, 128), 1).astype(F32)
    pad = jnp.zeros((128 - 24, 128), F32)
    for which in range(2):
        turned = jnp.transpose(jnp.concatenate([dense[which], pad], axis=0))
        for j in range(LOCAL_ROWS):
            spread = jnp.broadcast_to(turned[:, j : j + 1], (128, 128))
            at = (which * LOCAL_ROWS + j) * 128
            for g in range(8):
                hit = jnp.where(spread == column + float(128 * g), 1.0, 0.0)
                one_hot[at : at + 128, 128 * g : 128 * (g + 1)] = hit.astype(BF16)

    t_local[...] = jnp.zeros_like(t_local)
    t_rim[...] = jnp.zeros_like(t_rim)
    lhs_local[...] = jnp.zeros_like(lhs_local)
    lhs_rim[...] = jnp.zeros_like(lhs_rim)

    def load_six(ref):
        return jnp.concatenate([ref[0, 0, 0], jnp.zeros((2, GRAINS), F32)], axis=0)

    diag = load_six(diag_ref)
    field[0] = load_six(rhs_ref)

    def split_rows(source, target, chunk, at):
        whole = source[8 * chunk : 8 * chunk + 8, :]
        high = whole.astype(BF16).astype(F32)
        rest = whole - high
        mid = rest.astype(BF16).astype(F32)
        low_part = rest - mid
        cut = slice(128 * at, 128 * (at + 1))
        target[0:16, cut] = jnp.concatenate([high, mid], axis=0).astype(BF16)
        target[16:32, cut] = jnp.concatenate([low_part, jnp.zeros_like(low_part)], axis=0).astype(BF16)

    def scatter(lhs, hot):
        out = jnp.dot(lhs[...], hot[...], preferred_element_type=F32)
        return out[0:8] + out[8:16] + out[16:24]

    def local_forces(k):
        for v in range(3):
            rows = slice(8 * v, 8 * v + 8)
            ends = []
            for index_ref in (idx_a, idx_b):
                index = index_ref[rows, :]
                fine, coarse = index % 128, index // 128
                hits = [coarse == t for t in range(1, 8)]
                got = []
                for c in range(6):
                    total = lanes(splat(field[k, c : c + 1, 0:128]), fine)
                    for t in range(1, 8):
                        table = splat(field[k, c : c + 1, 128 * t : 128 * (t + 1)])
                        total = jnp.where(hits[t - 1], lanes(table, fine), total)
                    got.append(total)
                ends.append(got)
            first, second = response(
                ends[0], ends[1],
                [dense[3 + c, rows, :] for c in range(3)],
                dense[6, rows, :], dense[7, rows, :],
                [geo[q, rows, :] for q in range(4)], True,
            )
            for c in range(6):
                t_local[pl.ds(64 * v + c, 8, stride=8), :] = first[c]
                t_local[pl.ds(192 + 64 * v + c, 8, stride=8), :] = second[c]
        for which in range(2):
            for j in range(LOCAL_ROWS):
                split_rows(t_local, lhs_local, which * 24 + j, which * LOCAL_ROWS + j)
        return scatter(lhs_local, one_hot)

    def send_values(k):
        for v in range(4):
            rows = slice(8 * v, 8 * v + 8)
            index = rim_idx[rows, :]
            fine, upper = index % 128, index >= 128
            for pair in range(3):
                got = []
                for c in (2 * pair, 2 * pair + 1):
                    halves = [lanes(splat(field[k, c : c + 1, 128 * t : 128 * (t + 1)]), fine) for t in range(2)]
                    got.append(jnp.where(upper, halves[1], halves[0]))
                both = jnp.where(lane < 64, got[0], got[1])
                swapped = jnp.where(lane % 64 < 32, pltpu.roll(both, 96, 1), pltpu.roll(both, 32, 1))
                send_v[k, rows, pair, :] = swapped
                mine[pair, rows, :] = both
        copies = []
        for side in range(SIDES):
            copy = pltpu.make_async_remote_copy(
                src_ref=send_v.at[k, side + 2],
                dst_ref=recv_v.at[k, 27 - side],
                send_sem=v_send.at[k, side],
                recv_sem=v_recv.at[k, 25 - side],
                device_id=near[side],
                device_id_type=MESH,
            )
            copy.start()
            copies.append(copy)
        return copies

    def rim_forces(k):
        for v in range(4):
            rows = slice(8 * v, 8 * v + 8)
            a, b = [], []
            for pair in range(3):
                own = mine[pair, rows, :]
                got = recv_v[k, rows, pair, :]
                a += [own, pltpu.roll(own, 64, 1)]
                b += [got, pltpu.roll(got, 64, 1)]
            first, _ = response(
                a, b,
                [rim_geo[c, rows, :] for c in range(3)],
                rim_geo[3, rows, :], rim_geo[4, rows, :],
                [rim_geo[5 + q, rows, :] for q in range(4)], False,
            )
            for c in range(6):
                t_rim[pl.ds(64 * v + c, 8, stride=8), :] = first[c]
        for i in range(SIDES):
            split_rows(t_rim, lhs_rim, i + 2, i)
        return scatter(lhs_rim, rim_hot)

    sums = []

    def total_of(x):
        folded = x[:, 0:128]
        for t in range(1, 8):
            folded = folded + x[:, 128 * t : 128 * (t + 1)]
        return jnp.sum(folded, keepdims=True)

    lane_row = lane[0:1]

    def pack(values):
        out = jnp.zeros((1, 128), F32)
        for j, value in enumerate(values):
            out = jnp.where(lane_row == j, value, out)
        return out

    def spread(stage, where, buffer, rank, value):
        row_buf[stage] = value
        buffer[rank] = value
        copies = []
        for j, device in enumerate(where):
            copy = pltpu.make_async_remote_copy(
                src_ref=row_buf.at[stage],
                dst_ref=buffer.at[rank],
                send_sem=s_send.at[stage, j],
                recv_sem=s_recv.at[stage, j],
                device_id=device,
                device_id_type=MESH,
            )
            copy.start()
            copies.append(copy)
        return copies

    def gather_sum(copies, buffer, count):
        for copy in copies:
            copy.wait_recv()
        level = [buffer[j] for j in range(count)]
        while len(level) > 1:
            level = [level[j] + level[j + 1] for j in range(0, len(level), 2)]
        return level[0]

    def lane_of(values, j):
        return jnp.sum(jnp.where(lane_row == j, values, 0.0), keepdims=True)

    for copy in q_copies:
        copy.wait_recv()
    for v in range(4):
        rows = slice(8 * v, 8 * v + 8)
        seg = [rim_geo[q, rows, :] for q in range(8)]
        got = [recv_q[rows, h, :] for h in range(2)]

        def theirs(h, p):
            return lanes(got[h], lane % 32 + 32 * p)

        ours = lane % 64 >= 32
        valid = (lane < 64) & (row + 8 * v >= 2) & (row + 8 * v < 28)
        index = jnp.where(ours, seg[0], theirs(0, 0))
        kind = jnp.where(ours, seg[2], theirs(0, 1))
        rim_idx[rows, :] = index.astype(jnp.int32)
        for c in range(3):
            rim_geo[c, rows, :] = jnp.where(ours, seg[3 + c], -theirs(1, c))
        rim_geo[3, rows, :] = jnp.where(ours, seg[6], theirs(0, 3))
        rim_geo[4, rows, :] = jnp.where(ours, seg[7], theirs(0, 2))
        coeff = coefficients(kind, valid)
        for q in range(4):
            rim_geo[5 + q, rows, :] = coeff[q]

    sent = list(q_copies)
    copies = send_values(0)
    sent += copies
    index_rows = jnp.concatenate([rim_idx[...].astype(F32), jnp.zeros((96, 128), F32)], axis=0)
    turned = jnp.transpose(index_rows)
    for i in range(SIDES):
        spread_idx = jnp.broadcast_to(turned[:, i + 2 : i + 3], (128, 128))
        for g in range(2):
            hit = jnp.where(spread_idx == column + float(128 * g), 1.0, 0.0)
            rim_hot[128 * i : 128 * (i + 1), 128 * g : 128 * (g + 1)] = hit.astype(BF16)

    def apply(k, copies):
        whole = local_forces(k)
        for copy in copies:
            copy.wait_recv()
        rim = rim_forces(k)
        forces = jnp.concatenate([whole[:, :RIM] + rim, whole[:, RIM:]], axis=1)
        return diag * field[k] - forces

    w0 = field[0]
    w1 = apply(0, copies)
    field[1] = w1
    copies = send_values(1)
    sent += copies
    early = spread(0, plane, plane_buf.at[0], plane_rank, pack([total_of(w0 * w0), total_of(w0 * w1), total_of(w1 * w1)]))
    sent += early
    w2 = apply(1, copies)
    field[2] = w2
    copies = send_values(2)
    sent += copies
    early = spread(1, line, line_buf.at[0], line_rank, gather_sum(early, plane_buf.at[0], PLANE))
    sent += early
    w3 = apply(2, copies)
    early = gather_sum(early, line_buf.at[0], LINE)
    m0, m1, m2 = lane_of(early, 0), lane_of(early, 1), lane_of(early, 2)
    inv = jnp.sqrt(m0 / m2)
    shift = m1 / m0 * inv
    inv2 = inv * inv
    u0 = w0
    w1 = w1 * inv
    w2 = w2 * inv2
    w3 = w3 * (inv2 * inv)
    u1 = w1 - shift * u0
    u2 = w2 - shift * (2.0 * w1 - shift * u0)
    u3 = w3 - shift * (3.0 * w2 - shift * (3.0 * w1 - shift * u0))
    field[3] = u3
    copies = send_values(3)
    sent += copies
    basis = [u0, u1, u2, u3]
    pairs = [(0, 0), (0, 1), (1, 1), (1, 2), (2, 2), (2, 3), (3, 3)]
    known = [total_of(basis[i] * basis[j]) for i, j in pairs]
    u4 = apply(3, copies) * inv - shift * u3
    last = total_of(u3 * u4)
    late = spread(2, plane, plane_buf.at[1], plane_rank, pack(known + [last]))
    sent += late
    late = spread(3, line, line_buf.at[1], line_rank, gather_sum(late, plane_buf.at[1], PLANE))
    sent += late
    sums = gather_sum(late, line_buf.at[1], LINE)
    mu = [lane_of(sums, j) for j in range(8)]

    scale = 1.0 / inv

    def inner(p, q):
        by_degree = {}
        for i, x in enumerate(p):
            for j, y in enumerate(q):
                term = x * y
                by_degree[i + j] = by_degree[i + j] + term if i + j in by_degree else term
        out = None
        for degree, term in by_degree.items():
            term = term * mu[degree]
            out = term if out is None else out + term
        return out

    one = jnp.ones((1, 1), F32)
    res, direction, answer = [one], [one], []
    norm = mu[0]
    for step in range(4):
        image = [shift * direction[0]]
        for i in range(1, len(direction)):
            image.append(direction[i - 1] + shift * direction[i])
        image.append(direction[-1])
        image = [scale * value for value in image]
        alpha = norm / inner(direction, image)
        answer = [
            alpha * direction[i] + (answer[i] if i < len(answer) else 0.0)
            for i in range(len(direction))
        ]
        res = [
            (res[i] if i < len(res) else 0.0) - alpha * image[i]
            for i in range(len(image))
        ]
        if step < 3:
            fresh = inner(res, res)
            ratio = fresh / norm
            direction = [
                res[i] + (ratio * direction[i] if i < len(direction) else 0.0)
                for i in range(len(res))
            ]
            norm = fresh
    basis.append(u4)
    x = answer[0] * basis[0]
    for i in range(1, 4):
        x = x + answer[i] * basis[i]
    r = res[0] * basis[0]
    for i in range(1, 5):
        r = r + res[i] * basis[i]
    x_ref[0, 0, 0] = x[0:6]
    r_ref[0, 0, 0] = r[0:6]
    for copy in sent:
        copy.wait_send()


def shards(*arguments):
    vmem = pl.BlockSpec(memory_space=pltpu.VMEM)
    smem = pl.BlockSpec(memory_space=pltpu.SMEM)
    out = jax.ShapeDtypeStruct((1, 1, 1, 6, GRAINS), F32)
    dma = pltpu.SemaphoreType.DMA
    return pl.pallas_call(
        kernel,
        out_shape=(out, out),
        in_specs=[vmem, vmem, smem] + [vmem] * 5,
        out_specs=(vmem, vmem),
        scratch_shapes=[
            pltpu.VMEM((8, 24, 128), F32),
            pltpu.VMEM((24, 128), jnp.int32),
            pltpu.VMEM((24, 128), jnp.int32),
            pltpu.VMEM((4, 24, 128), F32),
            pltpu.VMEM((2 * LOCAL_ROWS * 128, GRAINS), BF16),
            pltpu.VMEM((2 * 24 * 8, 128), F32),
            pltpu.VMEM((32, 2 * LOCAL_ROWS * 128), BF16),
            pltpu.VMEM((32, 128), jnp.int32),
            pltpu.VMEM((9, 32, 128), F32),
            pltpu.VMEM((SIDES * 128, RIM), BF16),
            pltpu.VMEM((32 * 8, 128), F32),
            pltpu.VMEM((32, SIDES * 128), BF16),
            pltpu.VMEM((4, 8, GRAINS), F32),
            pltpu.VMEM((3, 32, 128), F32),
            pltpu.VMEM((32, 2, 128), F32),
            pltpu.VMEM((32, 2, 128), F32),
            pltpu.VMEM((4, 32, 3, 128), F32),
            pltpu.VMEM((4, 32, 3, 128), F32),
            pltpu.VMEM((4, 1, 128), F32),
            pltpu.VMEM((2, PLANE, 1, 128), F32),
            pltpu.VMEM((2, LINE, 1, 128), F32),
            dma((SIDES,)),
            dma((SIDES,)),
            dma((4, SIDES)),
            dma((4, SIDES)),
            dma((4, PLANE)),
            dma((4, PLANE)),
        ],
        compiler_params=pltpu.CompilerParams(
            collective_id=0, has_side_effects=True, vmem_limit_bytes=56 * 1024 * 1024
        ),
    )(*arguments)


def solution(mesh):
    placed = P("gx", "gy", "gz", None, None)
    flat = P("gx", "gy", "gz", None)
    return jax.shard_map(
        shards,
        mesh=mesh,
        in_specs=(placed, placed, P(), flat, flat, flat, placed, placed),
        out_specs=(placed, placed),
        check_vma=False,
    )
```

```python
import functools

import jax
import jax.numpy as jnp
from jax import lax
from jax.experimental import pallas as pl
from jax.experimental.pallas import tpu as pltpu
from jax.sharding import PartitionSpec as P

F32 = jnp.float32
BF16 = jnp.bfloat16
MESH = pl.DeviceIdType.MESH
GRAINS = 1024
RIM = 256
NEAR = 2240
TYPES = 4
SIDES = 26
LOCAL_ROWS = 18
NX, NY, NZ = 4, 8, 16
ZLO = 4
PLANE = 32
LINE = 16


def offset_of(side):
    whole = side + (1 if side >= 13 else 0)
    return (whole // 9 - 1, whole // 3 % 3 - 1, whole % 3 - 1)


def cross(w, n):
    return [
        w[1] * n[2] - w[2] * n[1],
        w[2] * n[0] - w[0] * n[2],
        w[0] * n[1] - w[1] * n[0],
    ]


def response(a, b, n, ra, rb, coeff, both):
    shear, normal_less, roll, twist_less = coeff
    arm = [rb * b[3 + c] + ra * a[3 + c] for c in range(3)]
    turn = cross(arm, n)
    delta = [b[c] - a[c] - turn[c] for c in range(3)]
    along = normal_less * (n[0] * delta[0] + n[1] * delta[1] + n[2] * delta[2])
    force = [shear * delta[c] + along * n[c] for c in range(3)]
    theta = [b[3 + c] - a[3 + c] for c in range(3)]
    twist = twist_less * (n[0] * theta[0] + n[1] * theta[1] + n[2] * theta[2])
    moment = [roll * theta[c] + twist * n[c] for c in range(3)]
    lever = cross(n, force)
    first = force + [ra * lever[c] + moment[c] for c in range(3)]
    if not both:
        return first, None
    second = [-f for f in force] + [rb * lever[c] - moment[c] for c in range(3)]
    return first, second


def lanes(x, index):
    return jnp.take_along_axis(x, index, axis=1, mode="promise_in_bounds")


def splat(row):
    return jnp.broadcast_to(row, (8, 128))


def kernel(
    rhs_ref, diag_ref, stiff_ref, own_ref, slot_ref, type_ref, normal_ref, radii_ref,
    x_ref,
    dense, idx_a, idx_b, geo, one_hot, t_local, lhs_local,
    rim_idx, rim_far, rim_geo, rim_hot, t_rim, lhs_rim, field, forces, mine,
    send_q, recv_q, send_v, recv_v, row_buf, plane_buf, line_buf,
    q_send, q_recv, v_send, v_recv, s_send, s_recv,
):
    gx, gy, gz = lax.axis_index("gx"), lax.axis_index("gy"), lax.axis_index("gz")
    wide, low = gz // ZLO, gz % ZLO

    near = []
    for side in range(SIDES):
        dx, dy, dz = offset_of(side)
        near.append(((gx + (dx + NX)) % NX, (gy + (dy + NY)) % NY, (gz + (dz + NZ)) % NZ))
    plane = []
    for j in range(1, PLANE):
        dy, dw = j // ZLO, j % ZLO
        plane.append((gx, (gy + dy) % NY, ((wide + dw) % ZLO) * ZLO + low))
    line = []
    for j in range(1, LINE):
        dx, dl = j // ZLO, j % ZLO
        line.append(((gx + dx) % NX, gy, wide * ZLO + (low + dl) % ZLO))
    plane_rank = gy * ZLO + wide
    line_rank = gx * ZLO + low

    lane = lax.broadcasted_iota(jnp.int32, (8, 128), 1)
    row = lax.broadcasted_iota(jnp.int32, (8, 128), 0)

    recv_q[0:2] = jnp.zeros((2, 14, 128), F32)
    recv_q[28:32] = jnp.zeros((4, 14, 128), F32)
    for e in range(3):
        recv_v[e, 0:2] = jnp.zeros((2, 3, 128), F32)
        recv_v[e, 28:32] = jnp.zeros((4, 3, 128), F32)

    barrier = pltpu.get_barrier_semaphore()
    for where in near + plane + line:
        pl.semaphore_signal(barrier, inc=1, device_id=where, device_id_type=MESH)

    dense[0] = own_ref[...].astype(F32)
    dense[1] = slot_ref[...].astype(F32)
    dense[2] = type_ref[...].astype(F32)
    for c in range(3):
        dense[3 + c] = normal_ref[24 * c : 24 * c + 24, :]
    for c in range(2):
        for i in range(24):
            dense[6 + c, i : i + 1, :] = radii_ref[0, 0, 0, c : c + 1, 128 * i : 128 * (i + 1)]

    def coefficients(kind, valid):
        out = []
        for q in range(4):
            total = jnp.zeros_like(kind)
            for t in range(TYPES):
                total = jnp.where(kind == float(t), stiff_ref[q, t], total)
            out.append(jnp.where(valid, total, 0.0))
        return [out[1], out[0] - out[1], out[2], out[3] - out[2]]

    def segments(q, v):
        low_row = dense[q, 17 + 2 * v : 18 + 2 * v, :]
        nxt = min(18 + 2 * v, 23)
        high_row = dense[q, nxt : nxt + 1, :]
        base = jnp.where(row < 4, splat(low_row), splat(high_row))
        return lanes(base, (lane % 32) + 32 * (row % 4))

    def quarter(parts):
        out = parts[3]
        for p in (2, 1, 0):
            out = jnp.where(lane < 32 * (p + 1), parts[p], out)
        return out

    kept = []
    for v in range(4):
        seg = [segments(q, v) for q in range(8)]
        side = (row + (8 * v - 2)).astype(F32)
        slot_rim = seg[1] - (GRAINS + RIM * side)
        rows = slice(8 * v, 8 * v + 8)
        send_q[rows, 12, :] = quarter([slot_rim, seg[2], seg[6], seg[7]])
        send_q[rows, 13, :] = quarter([seg[3], seg[4], seg[5], seg[0]])
        seg[1] = slot_rim
        kept.append(seg)
    for v in range(4):
        for q in range(8):
            rim_geo[q, 8 * v : 8 * v + 8, :] = kept[v][q]
    rim = jnp.concatenate([rhs_ref[8 * c : 8 * c + 2, :] for c in range(6)], axis=0)
    for side in range(SIDES):
        send_q[side + 2, 0:12, :] = rim

    pl.semaphore_wait(barrier, SIDES + PLANE - 1 + LINE - 1)

    q_copies = []
    for side in range(SIDES):
        copy = pltpu.make_async_remote_copy(
            src_ref=send_q.at[side + 2],
            dst_ref=recv_q.at[27 - side],
            send_sem=q_send.at[side],
            recv_sem=q_recv.at[25 - side],
            device_id=near[side],
            device_id_type=MESH,
        )
        copy.start()
        q_copies.append(copy)

    for v in range(3):
        rows = slice(8 * v, 8 * v + 8)
        number = (row + 8 * v) * 128 + lane
        inside = number < NEAR
        own = dense[0, rows, :]
        slot = jnp.where(inside, dense[1, rows, :], 0.0)
        idx_a[rows, :] = own.astype(jnp.int32)
        idx_b[rows, :] = slot.astype(jnp.int32)
        dense[1, rows, :] = slot
        coeff = coefficients(dense[2, rows, :], inside)
        for q in range(4):
            geo[q, rows, :] = coeff[q]

    column = lax.broadcasted_iota(jnp.int32, (128, 128), 1).astype(F32)
    pad = jnp.zeros((128 - 24, 128), F32)
    for which in range(2):
        turned = jnp.transpose(jnp.concatenate([dense[which], pad], axis=0))
        for j in range(LOCAL_ROWS):
            spread = jnp.broadcast_to(turned[:, j : j + 1], (128, 128))
            at = (which * LOCAL_ROWS + j) * 128
            for g in range(8):
                hit = jnp.where(spread == column + float(128 * g), 1.0, 0.0)
                one_hot[at : at + 128, 128 * g : 128 * (g + 1)] = hit.astype(BF16)

    def rim_rows(turned, first_row, at):
        for i in range(SIDES):
            spread_idx = jnp.broadcast_to(turned[first_row : first_row + 32, i + 2 : i + 3], (32, 128))
            start = 64 * i + at
            for g in range(2):
                hit = jnp.where(spread_idx == column[0:32] + float(128 * g), 1.0, 0.0)
                rim_hot[start : start + 32, 128 * g : 128 * (g + 1)] = hit.astype(BF16)

    rim_pad = jnp.zeros((96, 128), F32)
    rim_rows(jnp.transpose(jnp.concatenate([rim_geo[0], rim_pad], axis=0)), 0, 32)

    t_local[...] = jnp.zeros_like(t_local)
    t_rim[...] = jnp.zeros_like(t_rim)
    lhs_local[...] = jnp.zeros_like(lhs_local)
    lhs_rim[...] = jnp.zeros_like(lhs_rim)

    diag = diag_ref[...]
    field[0] = rhs_ref[...]

    def split_rows(whole, target, at):
        high = whole.astype(BF16).astype(F32)
        rest = whole - high
        mid = rest.astype(BF16).astype(F32)
        low_part = rest - mid
        cut = slice(128 * at, 128 * (at + 1))
        target[0:16, cut] = jnp.concatenate([high, mid], axis=0).astype(BF16)
        target[16:32, cut] = jnp.concatenate([low_part, jnp.zeros_like(low_part)], axis=0).astype(BF16)

    def scatter(lhs, hot):
        out = jnp.dot(lhs[...], hot[...], preferred_element_type=F32)
        return out[0:8] + out[8:16] + out[16:24]

    def local_forces(k):
        for v in range(3):
            rows = slice(8 * v, 8 * v + 8)
            ends = []
            for index_ref in (idx_a, idx_b):
                index = index_ref[rows, :]
                fine, coarse = index % 128, index // 128
                hits = [coarse == t for t in range(1, 8)]
                got = []
                for c in range(6):
                    total = lanes(splat(field[k, 8 * c : 8 * c + 1, :]), fine)
                    for t in range(1, 8):
                        table = splat(field[k, 8 * c + t : 8 * c + t + 1, :])
                        total = jnp.where(hits[t - 1], lanes(table, fine), total)
                    got.append(total)
                ends.append(got)
            first, second = response(
                ends[0], ends[1],
                [dense[3 + c, rows, :] for c in range(3)],
                dense[6, rows, :], dense[7, rows, :],
                [geo[q, rows, :] for q in range(4)], True,
            )
            for c in range(6):
                t_local[pl.ds(64 * v + c, 8, stride=8), :] = first[c]
                t_local[pl.ds(192 + 64 * v + c, 8, stride=8), :] = second[c]
        for which in range(2):
            for j in range(LOCAL_ROWS):
                start = 8 * (which * 24 + j)
                split_rows(t_local[start : start + 8, :], lhs_local, which * LOCAL_ROWS + j)
        return scatter(lhs_local, one_hot)

    def own_values(k, send):
        for v in range(4):
            rows = slice(8 * v, 8 * v + 8)
            index = rim_idx[rows, :]
            fine, upper = index % 128, index >= 128
            for pair in range(3):
                got = []
                for c in (2 * pair, 2 * pair + 1):
                    halves = [lanes(splat(field[k, 8 * c + t : 8 * c + t + 1, :]), fine) for t in range(2)]
                    got.append(jnp.where(upper, halves[1], halves[0]))
                both = jnp.where(lane < 64, got[0], got[1])
                mine[pair, rows, :] = both
                if send:
                    swapped = jnp.where(lane % 64 < 32, pltpu.roll(both, 96, 1), pltpu.roll(both, 32, 1))
                    send_v[k - 1, rows, pair, :] = swapped

    def send_values(k):
        own_values(k, True)
        copies = []
        for side in range(SIDES):
            copy = pltpu.make_async_remote_copy(
                src_ref=send_v.at[k - 1, side + 2],
                dst_ref=recv_v.at[k - 1, 27 - side],
                send_sem=v_send.at[k - 1, side],
                recv_sem=v_recv.at[k - 1, 25 - side],
                device_id=near[side],
                device_id_type=MESH,
            )
            copy.start()
            copies.append(copy)
        return copies

    def rim_forces(k):
        for v in range(4):
            rows = slice(8 * v, 8 * v + 8)
            a, b = [], []
            for pair in range(3):
                own = mine[pair, rows, :]
                a += [own, pltpu.roll(own, 64, 1)]
                if k > 0:
                    got = recv_v[k - 1, rows, pair, :]
                    b += [got, pltpu.roll(got, 64, 1)]
                else:
                    far = rim_far[rows, :]
                    for c in (2 * pair, 2 * pair + 1):
                        halves = [lanes(recv_q[rows, 2 * c + t, :], far % 128) for t in range(2)]
                        b.append(jnp.where(far >= 128, halves[1], halves[0]))
            first, _ = response(
                a, b,
                [rim_geo[c, rows, :] for c in range(3)],
                rim_geo[3, rows, :], rim_geo[4, rows, :],
                [rim_geo[5 + q, rows, :] for q in range(4)], False,
            )
            for c in range(6):
                t_rim[pl.ds(64 * v + c, 8, stride=8), :] = first[c]
        for i in range(SIDES // 2):
            start = 16 * (i + 1)
            even, odd = t_rim[start : start + 8, :], t_rim[start + 8 : start + 16, :]
            split_rows(jnp.where(lane < 64, even, pltpu.roll(odd, 64, 1)), lhs_rim, i)
        return scatter(lhs_rim, rim_hot)

    sums = []

    def total_of(x):
        folded = x[0:8]
        for t in range(1, 6):
            folded = folded + x[8 * t : 8 * t + 8]
        return jnp.sum(folded, keepdims=True)

    lane_row = lane[0:1]

    def pack(values):
        out = jnp.zeros((1, 128), F32)
        for j, value in enumerate(values):
            out = jnp.where(lane_row == j, value, out)
        return out

    def spread(stage, where, buffer, rank, value):
        row_buf[stage] = value
        buffer[rank] = value
        copies = []
        for j, device in enumerate(where):
            copy = pltpu.make_async_remote_copy(
                src_ref=row_buf.at[stage],
                dst_ref=buffer.at[rank],
                send_sem=s_send.at[stage, j],
                recv_sem=s_recv.at[stage, j],
                device_id=device,
                device_id_type=MESH,
            )
            copy.start()
            copies.append(copy)
        return copies

    def gather_sum(copies, buffer, count):
        for copy in copies:
            copy.wait_recv()
        level = [buffer[j] for j in range(count)]
        while len(level) > 1:
            level = [level[j] + level[j + 1] for j in range(0, len(level), 2)]
        return level[0]

    def lane_of(values, j):
        return jnp.sum(jnp.where(lane_row == j, values, 0.0), keepdims=True)

    def meet():
        for v in range(4):
            rows = slice(8 * v, 8 * v + 8)
            seg = [rim_geo[q, rows, :] for q in range(8)]
            got = [recv_q[rows, 12 + h, :] for h in range(2)]

            def theirs(h, p):
                return lanes(got[h], lane % 32 + 32 * p)

            ours = lane % 64 >= 32
            valid = (lane < 64) & (row + 8 * v >= 2) & (row + 8 * v < 28)
            index = jnp.where(ours, seg[0], theirs(0, 0))
            kind = jnp.where(ours, seg[2], theirs(0, 1))
            rim_idx[rows, :] = index.astype(jnp.int32)
            rim_far[rows, :] = jnp.where(ours, seg[1], theirs(1, 3)).astype(jnp.int32)
            for c in range(3):
                rim_geo[c, rows, :] = jnp.where(ours, seg[3 + c], -theirs(1, c))
            rim_geo[3, rows, :] = jnp.where(ours, seg[6], theirs(0, 3))
            rim_geo[4, rows, :] = jnp.where(ours, seg[7], theirs(0, 2))
            coeff = coefficients(kind, valid)
            for q in range(4):
                rim_geo[5 + q, rows, :] = coeff[q]
        own_values(0, False)
        turned = jnp.transpose(jnp.concatenate([rim_idx[...].astype(F32), rim_pad], axis=0))
        rim_rows(turned, 0, 0)

    sent = list(q_copies)

    def apply(k, copies):
        whole = local_forces(k)
        for copy in copies:
            copy.wait_recv()
        if k == 0:
            meet()
        rim = rim_forces(k)
        for t in range(8):
            part = whole[:, 128 * t : 128 * (t + 1)]
            if t < 2:
                part = part + rim[:, 128 * t : 128 * (t + 1)]
            forces[pl.ds(t, 8, stride=8), :] = part
        return diag * field[k] - forces[0:48, :]

    w0 = field[0]
    w1 = apply(0, q_copies)
    field[1] = w1
    copies = send_values(1)
    sent += copies
    early = spread(0, plane, plane_buf.at[0], plane_rank, pack([total_of(w0 * w0), total_of(w0 * w1), total_of(w1 * w1)]))
    sent += early
    w2 = apply(1, copies)
    field[2] = w2
    copies = send_values(2)
    sent += copies
    early = spread(1, line, line_buf.at[0], line_rank, gather_sum(early, plane_buf.at[0], PLANE))
    sent += early
    w3 = apply(2, copies)
    early = gather_sum(early, line_buf.at[0], LINE)
    m0, m1, m2 = lane_of(early, 0), lane_of(early, 1), lane_of(early, 2)
    inv = jnp.sqrt(m0 / m2)
    shift = m1 / m0 * inv
    inv2 = inv * inv
    u0 = w0
    w1 = w1 * inv
    w2 = w2 * inv2
    w3 = w3 * (inv2 * inv)
    u1 = w1 - shift * u0
    u2 = w2 - shift * (2.0 * w1 - shift * u0)
    u3 = w3 - shift * (3.0 * w2 - shift * (3.0 * w1 - shift * u0))
    field[3] = u3
    copies = send_values(3)
    sent += copies
    basis = [u0, u1, u2, u3]
    pairs = [(0, 0), (0, 1), (1, 1), (1, 2), (2, 2), (2, 3), (3, 3)]
    known = [total_of(basis[i] * basis[j]) for i, j in pairs]
    u4 = apply(3, copies) * inv - shift * u3
    last = total_of(u3 * u4)
    late = spread(2, plane, plane_buf.at[1], plane_rank, pack(known + [last]))
    sent += late
    late = spread(3, line, line_buf.at[1], line_rank, gather_sum(late, plane_buf.at[1], PLANE))
    sent += late
    sums = gather_sum(late, line_buf.at[1], LINE)
    mu = [lane_of(sums, j) for j in range(8)]

    scale = 1.0 / inv

    def inner(p, q):
        by_degree = {}
        for i, x in enumerate(p):
            for j, y in enumerate(q):
                term = x * y
                by_degree[i + j] = by_degree[i + j] + term if i + j in by_degree else term
        out = None
        for degree, term in by_degree.items():
            term = term * mu[degree]
            out = term if out is None else out + term
        return out

    one = jnp.ones((1, 1), F32)
    res, direction, answer = [one], [one], []
    norm = mu[0]
    for step in range(4):
        image = [shift * direction[0]]
        for i in range(1, len(direction)):
            image.append(direction[i - 1] + shift * direction[i])
        image.append(direction[-1])
        image = [scale * value for value in image]
        alpha = norm / inner(direction, image)
        answer = [
            alpha * direction[i] + (answer[i] if i < len(answer) else 0.0)
            for i in range(len(direction))
        ]
        res = [
            (res[i] if i < len(res) else 0.0) - alpha * image[i]
            for i in range(len(image))
        ]
        if step < 3:
            fresh = inner(res, res)
            ratio = fresh / norm
            direction = [
                res[i] + (ratio * direction[i] if i < len(direction) else 0.0)
                for i in range(len(res))
            ]
            norm = fresh
    basis.append(u4)
    x = answer[0] * basis[0]
    for i in range(1, 4):
        x = x + answer[i] * basis[i]
    r = res[0] * basis[0]
    for i in range(1, 5):
        r = r + res[i] * basis[i]
    x_ref[0:48] = x
    x_ref[48:96] = r
    for copy in sent:
        copy.wait_send()


def shards(*arguments):
    arguments = [
        x if x.ndim == 2 or x.shape[3] == 2 else x.reshape(x.size // 128, 128) for x in arguments
    ]
    vmem = pl.BlockSpec(memory_space=pltpu.VMEM)
    smem = pl.BlockSpec(memory_space=pltpu.SMEM)
    out = jax.ShapeDtypeStruct((48, 128), F32)
    dma = pltpu.SemaphoreType.DMA
    outs = pl.pallas_call(
        kernel,
        out_shape=jax.ShapeDtypeStruct((96,128),F32),
        in_specs=[vmem, vmem, smem] + [vmem] * 5,
        out_specs=vmem,
        scratch_shapes=[
            pltpu.VMEM((8, 24, 128), F32),
            pltpu.VMEM((24, 128), jnp.int32),
            pltpu.VMEM((24, 128), jnp.int32),
            pltpu.VMEM((4, 24, 128), F32),
            pltpu.VMEM((2 * LOCAL_ROWS * 128, GRAINS), BF16),
            pltpu.VMEM((2 * 24 * 8, 128), F32),
            pltpu.VMEM((32, 2 * LOCAL_ROWS * 128), BF16),
            pltpu.VMEM((32, 128), jnp.int32),
            pltpu.VMEM((32, 128), jnp.int32),
            pltpu.VMEM((9, 32, 128), F32),
            pltpu.VMEM((SIDES * 64, RIM), BF16),
            pltpu.VMEM((32 * 8, 128), F32),
            pltpu.VMEM((32, SIDES * 64), BF16),
            pltpu.VMEM((4, 48, 128), F32),
            pltpu.VMEM((64, 128), F32),
            pltpu.VMEM((3, 32, 128), F32),
            pltpu.VMEM((32, 14, 128), F32),
            pltpu.VMEM((32, 14, 128), F32),
            pltpu.VMEM((3, 32, 3, 128), F32),
            pltpu.VMEM((3, 32, 3, 128), F32),
            pltpu.VMEM((4, 1, 128), F32),
            pltpu.VMEM((2, PLANE, 1, 128), F32),
            pltpu.VMEM((2, LINE, 1, 128), F32),
            dma((SIDES,)),
            dma((SIDES,)),
            dma((3, SIDES)),
            dma((3, SIDES)),
            dma((4, PLANE)),
            dma((4, PLANE)),
        ],
        compiler_params=pltpu.CompilerParams(
            collective_id=0, has_side_effects=True, vmem_limit_bytes=56 * 1024 * 1024
        ),
    )(*arguments)
    return tuple(outs[48*i:48*i+48].reshape(1, 1, 1, 6, GRAINS) for i in range(2))


def solution(mesh):
    placed = P("gx", "gy", "gz", None, None)
    flat = P("gx", "gy", "gz", None)
    return jax.shard_map(
        shards,
        mesh=mesh,
        in_specs=(placed, placed, P(), flat, flat, flat, placed, placed),
        out_specs=(placed, placed),
        check_vma=False,
    )
```

```python
import functools

import jax
import jax.numpy as jnp
from jax import lax
from jax.experimental import pallas as pl
from jax.experimental.pallas import tpu as pltpu
from jax.sharding import PartitionSpec as P

F32 = jnp.float32
BF16 = jnp.bfloat16
MESH = pl.DeviceIdType.MESH
GRAINS = 1024
RIM = 256
NEAR = 2240
TYPES = 4
SIDES = 26
LOCAL_ROWS = 18
NX, NY, NZ = 4, 8, 16
ZLO = 4
PLANE = 32
LINE = 16


def offset_of(side):
    whole = side + (1 if side >= 13 else 0)
    return (whole // 9 - 1, whole // 3 % 3 - 1, whole % 3 - 1)


def cross(w, n):
    return [
        w[1] * n[2] - w[2] * n[1],
        w[2] * n[0] - w[0] * n[2],
        w[0] * n[1] - w[1] * n[0],
    ]


def response(a, b, n, ra, rb, coeff, both):
    shear, normal_less, roll, twist_less = coeff
    arm = [rb * b[3 + c] + ra * a[3 + c] for c in range(3)]
    turn = cross(arm, n)
    delta = [b[c] - a[c] - turn[c] for c in range(3)]
    along = normal_less * (n[0] * delta[0] + n[1] * delta[1] + n[2] * delta[2])
    force = [shear * delta[c] + along * n[c] for c in range(3)]
    theta = [b[3 + c] - a[3 + c] for c in range(3)]
    twist = twist_less * (n[0] * theta[0] + n[1] * theta[1] + n[2] * theta[2])
    moment = [roll * theta[c] + twist * n[c] for c in range(3)]
    lever = cross(n, force)
    first = force + [ra * lever[c] + moment[c] for c in range(3)]
    if not both:
        work = [force[c] * delta[c] + moment[c] * theta[c] for c in range(3)]
        return first, work[0] + work[1] + work[2]
    second = [-f for f in force] + [rb * lever[c] - moment[c] for c in range(3)]
    return first, second


def lanes(x, index):
    return jnp.take_along_axis(x, index, axis=1, mode="promise_in_bounds")


def splat(row):
    return jnp.broadcast_to(row, (8, 128))


def kernel(
    rhs_in, diag_in, stiff_in, own_in, slot_in, type_in, normal_in, radii_in,
    x_ref,
    rhs_ref, diag_ref, stiff_ref, own_ref, slot_ref, type_ref, normal_ref, radii_ref,
    dense, idx_a, idx_b, geo, one_hot, t_local, lhs_local,
    rim_idx, rim_far, rim_out, rim_geo, rim_hot, t_rim, lhs_rim, field, diag, mine,
    send_q, recv_q, send_v, recv_v, row_buf, plane_buf, line_buf,
    in_sem, q_send, q_recv, v_send, v_recv, s_send, s_recv,
):
    loads = []
    for j, (source, target) in enumerate((
        (rhs_in, rhs_ref), (own_in, own_ref), (slot_in, slot_ref), (type_in, type_ref),
        (normal_in, normal_ref), (radii_in.at[0, 0, 0], radii_ref), (stiff_in, stiff_ref),
        (diag_in, diag_ref),
    )):
        load = pltpu.make_async_copy(source, target, in_sem.at[j])
        load.start()
        loads.append(load)
    gx, gy, gz = lax.axis_index("gx"), lax.axis_index("gy"), lax.axis_index("gz")
    wide, low = gz // ZLO, gz % ZLO

    def distance(side):
        dx, dy, dz = offset_of(side)
        return (dx == 0, dx * dz >= 0, -abs(dz), -abs(dy))

    farthest_first = sorted(range(SIDES), key=distance)
    near = []
    for side in range(SIDES):
        dx, dy, dz = offset_of(side)
        near.append(((gx + (dx + NX)) % NX, (gy + (dy + NY)) % NY, (gz + (dz + NZ)) % NZ))
    plane = []
    for j in range(1, PLANE):
        dy, dw = j // ZLO, j % ZLO
        plane.append((gx, (gy + dy) % NY, ((wide + dw) % ZLO) * ZLO + low))
    line = []
    for j in range(1, LINE):
        dx, dl = j // ZLO, j % ZLO
        line.append(((gx + dx) % NX, gy, wide * ZLO + (low + dl) % ZLO))
    plane_rank = gy * ZLO + wide
    line_rank = gx * ZLO + low

    lane = lax.broadcasted_iota(jnp.int32, (8, 128), 1)
    row = lax.broadcasted_iota(jnp.int32, (8, 128), 0)

    barrier = pltpu.get_barrier_semaphore()
    for where in near + plane + line:
        pl.semaphore_signal(barrier, inc=1, device_id=where, device_id_type=MESH)

    recv_q[0:2] = jnp.zeros((2, 14, 128), F32)
    recv_q[28:32] = jnp.zeros((4, 14, 128), F32)
    for e in range(3):
        recv_v[e, 0:2] = jnp.zeros((2, 3, 128), F32)
        recv_v[e, 28:32] = jnp.zeros((4, 3, 128), F32)

    for load in loads:
        load.wait()

    dense[0] = own_ref[...].astype(F32)
    dense[1] = slot_ref[...].astype(F32)
    dense[2] = type_ref[...].astype(F32)
    for c in range(3):
        dense[3 + c] = normal_ref[24 * c : 24 * c + 24, :]
    for c in range(2):
        for i in range(24):
            dense[6 + c, i : i + 1, :] = radii_ref[c : c + 1, 128 * i : 128 * (i + 1)]

    stiffness = [
        [jnp.broadcast_to(stiff_ref[q : q + 1, t : t + 1], (8, 128)) for t in range(TYPES)]
        for q in range(4)
    ]

    def coefficients(kind, valid):
        out = []
        for q in range(4):
            total = jnp.zeros_like(kind)
            for t in range(TYPES):
                total = jnp.where(kind == float(t), stiffness[q][t], total)
            out.append(jnp.where(valid, total, 0.0))
        return [out[1], out[0] - out[1], out[2], out[3] - out[2]]

    def segments(q, v):
        low_row = dense[q, 17 + 2 * v : 18 + 2 * v, :]
        nxt = min(18 + 2 * v, 23)
        high_row = dense[q, nxt : nxt + 1, :]
        base = jnp.where(row < 4, splat(low_row), splat(high_row))
        return lanes(base, (lane % 32) + 32 * (row % 4))

    def quarter(parts):
        out = parts[3]
        for p in (2, 1, 0):
            out = jnp.where(lane < 32 * (p + 1), parts[p], out)
        return out

    kept = []
    for v in range(4):
        seg = [segments(q, v) for q in range(8)]
        side = (row + (8 * v - 2)).astype(F32)
        slot_rim = seg[1] - (GRAINS + RIM * side)
        rows = slice(8 * v, 8 * v + 8)
        send_q[rows, 12, :] = quarter([slot_rim, seg[2], seg[6], seg[7]])
        send_q[rows, 13, :] = quarter([seg[3], seg[4], seg[5], seg[0]])
        seg[1] = slot_rim
        kept.append(seg)
    for v in range(4):
        for q in range(8):
            rim_geo[q, 8 * v : 8 * v + 8, :] = kept[v][q]
    rim = jnp.concatenate([rhs_ref[8 * c : 8 * c + 2, :] for c in range(6)], axis=0)
    for side in range(SIDES):
        send_q[side + 2, 0:12, :] = rim

    pl.semaphore_wait(barrier, SIDES + PLANE - 1 + LINE - 1)

    q_copies = []
    for side in farthest_first:
        copy = pltpu.make_async_remote_copy(
            src_ref=send_q.at[side + 2],
            dst_ref=recv_q.at[27 - side],
            send_sem=q_send.at[side],
            recv_sem=q_recv.at[25 - side],
            device_id=near[side],
            device_id_type=MESH,
        )
        copy.start()
        q_copies.append(copy)

    for v in range(3):
        rows = slice(8 * v, 8 * v + 8)
        number = (row + 8 * v) * 128 + lane
        inside = number < NEAR
        own = dense[0, rows, :]
        slot = jnp.where(inside, dense[1, rows, :], 0.0)
        idx_a[rows, :] = own.astype(jnp.int32)
        idx_b[rows, :] = slot.astype(jnp.int32)
        dense[1, rows, :] = slot
        coeff = coefficients(dense[2, rows, :], inside)
        for q in range(4):
            geo[q, rows, :] = coeff[q]

    column = lax.broadcasted_iota(jnp.int32, (128, 128), 1).astype(F32)
    pad = jnp.zeros((128 - 24, 128), F32)
    for which in range(2):
        turned = jnp.transpose(jnp.concatenate([dense[which], pad], axis=0))
        for j in range(LOCAL_ROWS):
            spread = jnp.broadcast_to(turned[:, j : j + 1], (128, 128))
            at = (which * LOCAL_ROWS + j) * 128
            for g in range(8):
                hit = jnp.where(spread == column + float(128 * g), 1.0, 0.0)
                one_hot[at : at + 128, 128 * g : 128 * (g + 1)] = hit.astype(BF16)

    def rim_rows(turned, first_row, at):
        for i in range(SIDES):
            spread_idx = jnp.broadcast_to(turned[first_row : first_row + 32, i + 2 : i + 3], (32, 128))
            start = 64 * i + at
            for g in range(2):
                hit = jnp.where(spread_idx == column[0:32] + float(128 * g), 1.0, 0.0)
                rim_hot[start : start + 32, 128 * g : 128 * (g + 1)] = hit.astype(BF16)

    rim_pad = jnp.zeros((96, 128), F32)
    rim_rows(jnp.transpose(jnp.concatenate([rim_geo[0], rim_pad], axis=0)), 0, 32)

    t_local[...] = jnp.zeros_like(t_local)
    t_rim[...] = jnp.zeros_like(t_rim)
    lhs_local[...] = jnp.zeros_like(lhs_local)
    lhs_rim[...] = jnp.zeros_like(lhs_rim)

    field[0, 0:48, :] = rhs_ref[...]
    field[0, 48:64, :] = jnp.zeros((16, 128), F32)
    diag[0:48, :] = diag_ref[...]
    diag[48:64, :] = jnp.zeros((16, 128), F32)

    def split_rows(whole, target, at):
        high = whole.astype(BF16).astype(F32)
        rest = whole - high
        mid = rest.astype(BF16).astype(F32)
        low_part = rest - mid
        cut = slice(128 * at, 128 * (at + 1))
        target[0:16, cut] = jnp.concatenate([high, mid], axis=0).astype(BF16)
        target[16:32, cut] = jnp.concatenate([low_part, jnp.zeros_like(low_part)], axis=0).astype(BF16)

    def scatter(lhs, hot):
        out = jnp.dot(lhs[...], hot[...], preferred_element_type=F32)
        return out[0:8] + out[8:16] + out[16:24]

    def local_forces(k):
        for v in range(3):
            rows = slice(8 * v, 8 * v + 8)
            ends = []
            for index_ref in (idx_a, idx_b):
                index = index_ref[rows, :]
                fine, coarse = index % 128, index // 128
                hits = [coarse == t for t in range(1, 8)]
                got = []
                for c in range(6):
                    total = lanes(splat(field[k, 8 * c : 8 * c + 1, :]), fine)
                    for t in range(1, 8):
                        table = splat(field[k, 8 * c + t : 8 * c + t + 1, :])
                        total = jnp.where(hits[t - 1], lanes(table, fine), total)
                    got.append(total)
                ends.append(got)
            first, second = response(
                ends[0], ends[1],
                [dense[3 + c, rows, :] for c in range(3)],
                dense[6, rows, :], dense[7, rows, :],
                [geo[q, rows, :] for q in range(4)], True,
            )
            for c in range(6):
                t_local[pl.ds(64 * v + c, 8, stride=8), :] = first[c]
                t_local[pl.ds(192 + 64 * v + c, 8, stride=8), :] = second[c]
        for which in range(2):
            for j in range(LOCAL_ROWS):
                start = 8 * (which * 24 + j)
                split_rows(t_local[start : start + 8, :], lhs_local, which * LOCAL_ROWS + j)
        return scatter(lhs_local, one_hot)

    def rim_values(k, index_ref, v):
        index = index_ref[8 * v : 8 * v + 8, :]
        fine, upper = index % 128, index >= 128
        out = []
        for pair in range(3):
            got = []
            for c in (2 * pair, 2 * pair + 1):
                halves = [lanes(splat(field[k, 8 * c + t : 8 * c + t + 1, :]), fine) for t in range(2)]
                got.append(jnp.where(upper, halves[1], halves[0]))
            out.append(jnp.where(lane < 64, got[0], got[1]))
        return out

    def own_values(k):
        for v in range(4):
            got = rim_values(k, rim_idx, v)
            for pair in range(3):
                mine[pair, 8 * v : 8 * v + 8, :] = got[pair]

    def send_values(k):
        for v in range(4):
            got = rim_values(k, rim_out, v)
            for pair in range(3):
                send_v[k - 1, 8 * v : 8 * v + 8, pair, :] = got[pair]
        copies = []
        for side in farthest_first:
            copy = pltpu.make_async_remote_copy(
                src_ref=send_v.at[k - 1, side + 2],
                dst_ref=recv_v.at[k - 1, 27 - side],
                send_sem=v_send.at[k - 1, side],
                recv_sem=v_recv.at[k - 1, 25 - side],
                device_id=near[side],
                device_id_type=MESH,
            )
            copy.start()
            copies.append(copy)
        own_values(k)
        return copies

    def rim_contacts(k):
        work = jnp.zeros((8, 128), F32)
        for v in range(4):
            rows = slice(8 * v, 8 * v + 8)
            a, b = [], []
            for pair in range(3):
                own = mine[pair, rows, :]
                a += [own, pltpu.roll(own, 64, 1)]
                if k > 0:
                    got = recv_v[k - 1, rows, pair, :]
                    b += [got, pltpu.roll(got, 64, 1)]
                else:
                    far = rim_far[rows, :]
                    for c in (2 * pair, 2 * pair + 1):
                        halves = [lanes(recv_q[rows, 2 * c + t, :], far % 128) for t in range(2)]
                        b.append(jnp.where(far >= 128, halves[1], halves[0]))
            first, done = response(
                a, b,
                [rim_geo[c, rows, :] for c in range(3)],
                rim_geo[3, rows, :], rim_geo[4, rows, :],
                [rim_geo[5 + q, rows, :] for q in range(4)], False,
            )
            for c in range(6):
                t_rim[pl.ds(64 * v + c, 8, stride=8), :] = first[c]
            work = work + done
        return jnp.sum(jnp.where(lane >= 32, work, 0.0), keepdims=True)

    def rim_forces():
        for i in range(SIDES // 2):
            start = 16 * (i + 1)
            even, odd = t_rim[start : start + 8, :], t_rim[start + 8 : start + 16, :]
            split_rows(jnp.where(lane < 64, even, pltpu.roll(odd, 64, 1)), lhs_rim, i)
        return scatter(lhs_rim, rim_hot)

    sums = []

    def total_of(x):
        folded = x[0:8]
        for t in range(1, 6):
            folded = folded + x[8 * t : 8 * t + 8]
        return jnp.sum(folded, keepdims=True)

    lane_row = lane[0:1]

    def pack(values):
        out = jnp.zeros((1, 128), F32)
        for j, value in enumerate(values):
            out = jnp.where(lane_row == j, value, out)
        return out

    def spread(stage, where, buffer, rank, value):
        row_buf[stage] = value
        buffer[rank] = value
        copies = []
        for j, device in enumerate(where):
            copy = pltpu.make_async_remote_copy(
                src_ref=row_buf.at[stage],
                dst_ref=buffer.at[rank],
                send_sem=s_send.at[stage, j],
                recv_sem=s_recv.at[stage, j],
                device_id=device,
                device_id_type=MESH,
            )
            copy.start()
            copies.append(copy)
        return copies

    def gather_sum(copies, buffer, count):
        for copy in copies:
            copy.wait_recv()
        level = [buffer[j] for j in range(count)]
        while len(level) > 1:
            level = [level[j] + level[j + 1] for j in range(0, len(level), 2)]
        return level[0]

    def lane_of(values, j):
        return jnp.sum(jnp.where(lane_row == j, values, 0.0), keepdims=True)

    def meet():
        for v in range(4):
            rows = slice(8 * v, 8 * v + 8)
            seg = [rim_geo[q, rows, :] for q in range(8)]
            got = [recv_q[rows, 12 + h, :] for h in range(2)]

            def theirs(h, p):
                return lanes(got[h], lane % 32 + 32 * p)

            ours = lane % 64 >= 32
            valid = (lane < 64) & (row + 8 * v >= 2) & (row + 8 * v < 28)
            index = jnp.where(ours, seg[0], theirs(0, 0))
            kind = jnp.where(ours, seg[2], theirs(0, 1))
            rim_idx[rows, :] = index.astype(jnp.int32)
            flipped = jnp.where(ours, theirs(0, 0), seg[0])
            rim_out[rows, :] = flipped.astype(jnp.int32)
            rim_far[rows, :] = jnp.where(ours, seg[1], theirs(1, 3)).astype(jnp.int32)
            for c in range(3):
                rim_geo[c, rows, :] = jnp.where(ours, seg[3 + c], -theirs(1, c))
            rim_geo[3, rows, :] = jnp.where(ours, seg[6], theirs(0, 3))
            rim_geo[4, rows, :] = jnp.where(ours, seg[7], theirs(0, 2))
            coeff = coefficients(kind, valid)
            for q in range(4):
                rim_geo[5 + q, rows, :] = coeff[q]
        own_values(0)
        turned = jnp.transpose(jnp.concatenate([rim_idx[...].astype(F32), rim_pad], axis=0))
        rim_rows(turned, 0, 0)

    sent = list(q_copies)

    def tile(ref, t):
        return ref[pl.ds(t, 8, stride=8), :]

    def product(k, t, forces):
        return tile(diag, t) * tile(field.at[k], t) - forces

    def apply(k, copies, finish, between=None):
        whole = local_forces(k)
        if between is not None:
            between()
        for t in range(2, 8):
            field[k + 1, pl.ds(t, 8, stride=8), :] = finish(product(k, t, whole[:, 128 * t : 128 * (t + 1)]), t)
        start = [product(k, t, whole[:, 128 * t : 128 * (t + 1)]) for t in range(2)]
        for copy in copies:
            copy.wait_recv()
        if k == 0:
            meet()
        rim_contacts(k)
        rim = rim_forces()
        for t in range(2):
            value = start[t] - rim[:, 128 * t : 128 * (t + 1)]
            field[k + 1, pl.ds(t, 8, stride=8), :] = finish(value, t)
        out = send_values(k + 1)
        sent.extend(out)
        return out

    def plain(value, t):
        return value

    def dense_of(k):
        return field[k, 0:48, :]

    w0 = dense_of(0)
    copies = apply(0, q_copies, plain)
    w1 = dense_of(1)
    first_sums = pack([total_of(w0 * w0), total_of(w0 * w1), total_of(w1 * w1)])
    early = spread(0, plane, plane_buf.at[0], plane_rank, first_sums)
    sent += early
    held = {}

    def onward():
        held["line"] = spread(1, line, line_buf.at[0], line_rank, gather_sum(early, plane_buf.at[0], PLANE))
        sent.extend(held["line"])

    copies = apply(1, copies, plain, onward)

    def settle():
        total = gather_sum(held["line"], line_buf.at[0], LINE)
        m0, m1, m2 = lane_of(total, 0), lane_of(total, 1), lane_of(total, 2)
        held["inv"] = jnp.sqrt(m0 / m2)
        held["shift"] = m1 / m0 * held["inv"]

    def centred(value, t):
        inv, shift = held["inv"], held["shift"]
        inv2 = inv * inv
        b, p, q = [tile(field.at[j], t) for j in range(3)]
        p, q = p * inv, q * inv2
        return value * (inv2 * inv) - shift * (3.0 * q - shift * (3.0 * p - shift * b))

    copies = apply(2, copies, centred, settle)
    inv, shift = held["inv"], held["shift"]
    u0, u3 = w0, dense_of(3)
    p, q = w1 * inv, dense_of(2) * (inv * inv)
    u1 = p - shift * u0
    u2 = q - shift * (2.0 * p - shift * u0)
    basis = [u0, u1, u2, u3]
    pairs = [(0, 0), (0, 1), (1, 1), (1, 2), (2, 2), (2, 3), (3, 3)]
    known = [total_of(basis[i] * basis[j]) for i, j in pairs]
    whole = local_forces(3)
    near_work = jnp.zeros((8, 128), F32)
    for t in range(8):
        value = product(3, t, whole[:, 128 * t : 128 * (t + 1)])
        field[4, pl.ds(t, 8, stride=8), :] = value
        near_work = near_work + value * tile(field.at[3], t)
    near_work = inv * jnp.sum(near_work, keepdims=True) - shift * known[6]
    for copy in copies:
        copy.wait_recv()
    last = near_work + inv * rim_contacts(3)
    late = spread(2, plane, plane_buf.at[1], plane_rank, pack(known + [last]))
    sent += late
    rim = rim_forces()
    for t in range(2):
        value = tile(field.at[4], t) - rim[:, 128 * t : 128 * (t + 1)]
        field[4, pl.ds(t, 8, stride=8), :] = value
    u4 = dense_of(4) * inv - shift * u3
    late = spread(3, line, line_buf.at[1], line_rank, gather_sum(late, plane_buf.at[1], PLANE))
    sent += late
    sums = gather_sum(late, line_buf.at[1], LINE)
    mu = [lane_of(sums, j) for j in range(8)]

    scale = 1.0 / inv

    def inner(p, q):
        by_degree = {}
        for i, x in enumerate(p):
            for j, y in enumerate(q):
                term = x * y
                by_degree[i + j] = by_degree[i + j] + term if i + j in by_degree else term
        out = None
        for degree, term in by_degree.items():
            term = term * mu[degree]
            out = term if out is None else out + term
        return out

    one = jnp.ones((1, 1), F32)
    res, direction, answer = [one], [one], []
    norm = mu[0]
    for step in range(4):
        image = [shift * direction[0]]
        for i in range(1, len(direction)):
            image.append(direction[i - 1] + shift * direction[i])
        image.append(direction[-1])
        image = [scale * value for value in image]
        alpha = norm / inner(direction, image)
        answer = [
            alpha * direction[i] + (answer[i] if i < len(answer) else 0.0)
            for i in range(len(direction))
        ]
        res = [
            (res[i] if i < len(res) else 0.0) - alpha * image[i]
            for i in range(len(image))
        ]
        if step < 3:
            fresh = inner(res, res)
            ratio = fresh / norm
            direction = [
                res[i] + (ratio * direction[i] if i < len(direction) else 0.0)
                for i in range(len(res))
            ]
            norm = fresh
    basis.append(u4)
    x = answer[0] * basis[0]
    for i in range(1, 4):
        x = x + answer[i] * basis[i]
    r = res[0] * basis[0]
    for i in range(1, 5):
        r = r + res[i] * basis[i]
    x_ref[0:48] = x
    x_ref[48:96] = r
    for copy in sent:
        copy.wait_send()


def shards(*arguments):
    arguments = [
        x if x.ndim == 2 or x.shape[3] == 2 else x.reshape(x.size // 128, 128) for x in arguments
    ]
    vmem = pl.BlockSpec(memory_space=pltpu.VMEM)
    hbm = pl.BlockSpec(memory_space=pltpu.HBM)
    out = jax.ShapeDtypeStruct((48, 128), F32)
    dma = pltpu.SemaphoreType.DMA
    outs = pl.pallas_call(
        kernel,
        out_shape=jax.ShapeDtypeStruct((96,128),F32),
        in_specs=[hbm] * 8,
        out_specs=vmem,
        scratch_shapes=[
            pltpu.VMEM((48, 128), F32),
            pltpu.VMEM((48, 128), F32),
            pltpu.VMEM((4, 4), F32),
            pltpu.VMEM((24, 128), jnp.int32),
            pltpu.VMEM((24, 128), jnp.int32),
            pltpu.VMEM((24, 128), jnp.int32),
            pltpu.VMEM((72, 128), F32),
            pltpu.VMEM((2, 3072), F32),
            pltpu.VMEM((8, 24, 128), F32),
            pltpu.VMEM((24, 128), jnp.int32),
            pltpu.VMEM((24, 128), jnp.int32),
            pltpu.VMEM((4, 24, 128), F32),
            pltpu.VMEM((2 * LOCAL_ROWS * 128, GRAINS), BF16),
            pltpu.VMEM((2 * 24 * 8, 128), F32),
            pltpu.VMEM((32, 2 * LOCAL_ROWS * 128), BF16),
            pltpu.VMEM((32, 128), jnp.int32),
            pltpu.VMEM((32, 128), jnp.int32),
            pltpu.VMEM((32, 128), jnp.int32),
            pltpu.VMEM((9, 32, 128), F32),
            pltpu.VMEM((SIDES * 64, RIM), BF16),
            pltpu.VMEM((32 * 8, 128), F32),
            pltpu.VMEM((32, SIDES * 64), BF16),
            pltpu.VMEM((5, 64, 128), F32),
            pltpu.VMEM((64, 128), F32),
            pltpu.VMEM((3, 32, 128), F32),
            pltpu.VMEM((32, 14, 128), F32),
            pltpu.VMEM((32, 14, 128), F32),
            pltpu.VMEM((3, 32, 3, 128), F32),
            pltpu.VMEM((3, 32, 3, 128), F32),
            pltpu.VMEM((4, 1, 128), F32),
            pltpu.VMEM((2, PLANE, 1, 128), F32),
            pltpu.VMEM((2, LINE, 1, 128), F32),
            dma((8,)),
            dma((SIDES,)),
            dma((SIDES,)),
            dma((3, SIDES)),
            dma((3, SIDES)),
            dma((4, PLANE)),
            dma((4, PLANE)),
        ],
        compiler_params=pltpu.CompilerParams(
            collective_id=0, has_side_effects=True, vmem_limit_bytes=56 * 1024 * 1024
        ),
    )(*arguments)
    return tuple(outs[48*i:48*i+48].reshape(1, 1, 1, 6, GRAINS) for i in range(2))


def solution(mesh):
    placed = P("gx", "gy", "gz", None, None)
    flat = P("gx", "gy", "gz", None)
    return jax.shard_map(
        shards,
        mesh=mesh,
        in_specs=(placed, placed, P(), flat, flat, flat, placed, placed),
        out_specs=(placed, placed),
        check_vma=False,
    )
```

```python
import functools

import jax
import jax.numpy as jnp
from jax import lax
from jax.experimental import pallas as pl
from jax.experimental.pallas import tpu as pltpu
from jax.sharding import PartitionSpec as P

F32 = jnp.float32
BF16 = jnp.bfloat16
MESH = pl.DeviceIdType.MESH
GRAINS = 1024
RIM = 256
NEAR = 2240
TYPES = 4
SIDES = 26
LOCAL_ROWS = 18
NX, NY, NZ = 4, 8, 16
ZLO = 4
PLANE = 32
LINE = 16


def offset_of(side):
    whole = side + (1 if side >= 13 else 0)
    return (whole // 9 - 1, whole // 3 % 3 - 1, whole % 3 - 1)


def cross(w, n):
    return [
        w[1] * n[2] - w[2] * n[1],
        w[2] * n[0] - w[0] * n[2],
        w[0] * n[1] - w[1] * n[0],
    ]


def response(a, b, n, ra, rb, coeff, both):
    shear, normal_less, roll, twist_less = coeff
    arm = [rb * b[3 + c] + ra * a[3 + c] for c in range(3)]
    turn = cross(arm, n)
    delta = [b[c] - a[c] - turn[c] for c in range(3)]
    along = normal_less * (n[0] * delta[0] + n[1] * delta[1] + n[2] * delta[2])
    force = [shear * delta[c] + along * n[c] for c in range(3)]
    theta = [b[3 + c] - a[3 + c] for c in range(3)]
    twist = twist_less * (n[0] * theta[0] + n[1] * theta[1] + n[2] * theta[2])
    moment = [roll * theta[c] + twist * n[c] for c in range(3)]
    lever = cross(n, force)
    first = force + [ra * lever[c] + moment[c] for c in range(3)]
    if not both:
        work = [force[c] * delta[c] + moment[c] * theta[c] for c in range(3)]
        return first, work[0] + work[1] + work[2]
    second = [-f for f in force] + [rb * lever[c] - moment[c] for c in range(3)]
    return first, second


def lanes(x, index):
    return jnp.take_along_axis(x, index, axis=1, mode="promise_in_bounds")


def splat(row):
    return jnp.broadcast_to(row, (8, 128))


def kernel(
    rhs_in, diag_in, stiff_in, own_in, slot_in, type_in, normal_in, radii_in,
    x_ref,
    rhs_ref, diag_ref, stiff_ref, own_ref, slot_ref, type_ref, normal_ref, radii_ref,
    dense, idx_a, idx_b, geo, one_hot, t_local, lhs_local,
    rim_idx, rim_far, rim_out, rim_geo, rim_hot, t_rim, lhs_rim, field, diag, mine,
    send_q, recv_q, send_v, recv_v, row_buf, plane_buf, line_buf,
    in_sem, q_send, q_recv, v_send, v_recv, s_send, s_recv,
):
    loads = []
    for j, (source, target) in enumerate((
        (rhs_in, rhs_ref), (own_in, own_ref), (slot_in, slot_ref), (type_in, type_ref),
        (normal_in, normal_ref), (radii_in.at[0, 0, 0], radii_ref), (stiff_in, stiff_ref),
        (diag_in, diag_ref),
    )):
        load = pltpu.make_async_copy(source, target, in_sem.at[j])
        load.start()
        loads.append(load)
    gx, gy, gz = lax.axis_index("gx"), lax.axis_index("gy"), lax.axis_index("gz")
    wide, low = gz // ZLO, gz % ZLO

    def distance(side):
        dx, dy, dz = offset_of(side)
        return (dx == 0, dx * dz >= 0, -abs(dz), -abs(dy))

    farthest_first = sorted(range(SIDES), key=distance)
    near = []
    for side in range(SIDES):
        dx, dy, dz = offset_of(side)
        near.append(((gx + (dx + NX)) % NX, (gy + (dy + NY)) % NY, (gz + (dz + NZ)) % NZ))
    plane = []
    for j in range(1, PLANE):
        dy, dw = j // ZLO, j % ZLO
        plane.append((gx, (gy + dy) % NY, ((wide + dw) % ZLO) * ZLO + low))
    line = []
    for j in range(1, LINE):
        dx, dl = j // ZLO, j % ZLO
        line.append(((gx + dx) % NX, gy, wide * ZLO + (low + dl) % ZLO))
    plane_rank = gy * ZLO + wide
    line_rank = gx * ZLO + low

    lane = lax.broadcasted_iota(jnp.int32, (8, 128), 1)
    row = lax.broadcasted_iota(jnp.int32, (8, 128), 0)

    barrier = pltpu.get_barrier_semaphore()
    for where in near + plane + line:
        pl.semaphore_signal(barrier, inc=1, device_id=where, device_id_type=MESH)

    recv_q[0:2] = jnp.zeros((2, 14, 128), F32)
    recv_q[28:32] = jnp.zeros((4, 14, 128), F32)
    for e in range(3):
        recv_v[e, 0:2] = jnp.zeros((2, 3, 128), F32)
        recv_v[e, 28:32] = jnp.zeros((4, 3, 128), F32)

    for load in loads:
        load.wait()

    dense[0] = own_ref[...].astype(F32)
    dense[1] = slot_ref[...].astype(F32)
    dense[2] = type_ref[...].astype(F32)
    for c in range(3):
        dense[3 + c] = normal_ref[24 * c : 24 * c + 24, :]
    for c in range(2):
        for i in range(24):
            dense[6 + c, i : i + 1, :] = radii_ref[c : c + 1, 128 * i : 128 * (i + 1)]

    stiffness = [
        [jnp.broadcast_to(stiff_ref[q : q + 1, t : t + 1], (8, 128)) for t in range(TYPES)]
        for q in range(4)
    ]

    def coefficients(kind, valid):
        out = []
        for q in range(4):
            total = jnp.zeros_like(kind)
            for t in range(TYPES):
                total = jnp.where(kind == float(t), stiffness[q][t], total)
            out.append(jnp.where(valid, total, 0.0))
        return [out[1], out[0] - out[1], out[2], out[3] - out[2]]

    def segments(q, v):
        low_row = dense[q, 17 + 2 * v : 18 + 2 * v, :]
        nxt = min(18 + 2 * v, 23)
        high_row = dense[q, nxt : nxt + 1, :]
        base = jnp.where(row < 4, splat(low_row), splat(high_row))
        return lanes(base, (lane % 32) + 32 * (row % 4))

    def quarter(parts):
        out = parts[3]
        for p in (2, 1, 0):
            out = jnp.where(lane < 32 * (p + 1), parts[p], out)
        return out

    kept = []
    for v in range(4):
        seg = [segments(q, v) for q in range(8)]
        side = (row + (8 * v - 2)).astype(F32)
        slot_rim = seg[1] - (GRAINS + RIM * side)
        rows = slice(8 * v, 8 * v + 8)
        send_q[rows, 12, :] = quarter([slot_rim, seg[2], seg[6], seg[7]])
        send_q[rows, 13, :] = quarter([seg[3], seg[4], seg[5], seg[0]])
        seg[1] = slot_rim
        kept.append(seg)
    for v in range(4):
        for q in range(8):
            rim_geo[q, 8 * v : 8 * v + 8, :] = kept[v][q]
    rim = jnp.concatenate([rhs_ref[8 * c : 8 * c + 2, :] for c in range(6)], axis=0)
    for side in range(SIDES):
        send_q[side + 2, 0:12, :] = rim

    pl.semaphore_wait(barrier, SIDES + PLANE - 1 + LINE - 1)

    q_copies = []
    for side in farthest_first:
        copy = pltpu.make_async_remote_copy(
            src_ref=send_q.at[side + 2],
            dst_ref=recv_q.at[27 - side],
            send_sem=q_send.at[side],
            recv_sem=q_recv.at[25 - side],
            device_id=near[side],
            device_id_type=MESH,
        )
        copy.start()
        q_copies.append(copy)

    for v in range(3):
        rows = slice(8 * v, 8 * v + 8)
        number = (row + 8 * v) * 128 + lane
        inside = number < NEAR
        own = dense[0, rows, :]
        slot = jnp.where(inside, dense[1, rows, :], 0.0)
        idx_a[rows, :] = own.astype(jnp.int32)
        idx_b[rows, :] = slot.astype(jnp.int32)
        dense[1, rows, :] = slot
        coeff = coefficients(dense[2, rows, :], inside)
        for q in range(4):
            geo[q, rows, :] = coeff[q]

    column = lax.broadcasted_iota(jnp.int32, (128, 128), 1).astype(F32)
    pad = jnp.zeros((128 - 24, 128), F32)
    for which in range(2):
        turned = jnp.transpose(jnp.concatenate([dense[which], pad], axis=0))
        for j in range(LOCAL_ROWS):
            spread = jnp.broadcast_to(turned[:, j : j + 1], (128, 128))
            at = (which * LOCAL_ROWS + j) * 128
            for g in range(8):
                hit = jnp.where(spread == column + float(128 * g), 1.0, 0.0)
                one_hot[at : at + 128, 128 * g : 128 * (g + 1)] = hit.astype(BF16)

    def rim_rows(turned, first_row, at):
        for i in range(SIDES):
            spread_idx = jnp.broadcast_to(turned[first_row : first_row + 32, i + 2 : i + 3], (32, 128))
            start = 64 * i + at
            for g in range(2):
                hit = jnp.where(spread_idx == column[0:32] + float(128 * g), 1.0, 0.0)
                rim_hot[start : start + 32, 128 * g : 128 * (g + 1)] = hit.astype(BF16)

    rim_pad = jnp.zeros((96, 128), F32)
    rim_rows(jnp.transpose(jnp.concatenate([rim_geo[0], rim_pad], axis=0)), 0, 32)

    t_local[...] = jnp.zeros_like(t_local)
    t_rim[...] = jnp.zeros_like(t_rim)
    lhs_local[...] = jnp.zeros_like(lhs_local)
    lhs_rim[...] = jnp.zeros_like(lhs_rim)

    field[0, 0:48, :] = rhs_ref[...]
    field[0, 48:64, :] = jnp.zeros((16, 128), F32)
    diag[0:48, :] = diag_ref[...]
    diag[48:64, :] = jnp.zeros((16, 128), F32)

    def split_rows(whole, target, at):
        high = whole.astype(BF16).astype(F32)
        rest = whole - high
        mid = rest.astype(BF16).astype(F32)
        low_part = rest - mid
        cut = slice(128 * at, 128 * (at + 1))
        target[0:16, cut] = jnp.concatenate([high, mid], axis=0).astype(BF16)
        target[16:32, cut] = jnp.concatenate([low_part, jnp.zeros_like(low_part)], axis=0).astype(BF16)

    def scatter(lhs, hot):
        out = jnp.dot(lhs[...], hot[...], preferred_element_type=F32)
        return out[0:8] + out[8:16] + out[16:24]

    def local_forces(k):
        for v in range(3):
            rows = slice(8 * v, 8 * v + 8)
            ends = []
            for index_ref in (idx_a, idx_b):
                index = index_ref[rows, :]
                fine, coarse = index % 128, index // 128
                hits = [coarse == t for t in range(1, 8)]
                got = []
                for c in range(6):
                    total = lanes(splat(field[k, 8 * c : 8 * c + 1, :]), fine)
                    for t in range(1, 8):
                        table = splat(field[k, 8 * c + t : 8 * c + t + 1, :])
                        total = jnp.where(hits[t - 1], lanes(table, fine), total)
                    got.append(total)
                ends.append(got)
            first, second = response(
                ends[0], ends[1],
                [dense[3 + c, rows, :] for c in range(3)],
                dense[6, rows, :], dense[7, rows, :],
                [geo[q, rows, :] for q in range(4)], True,
            )
            for c in range(6):
                t_local[pl.ds(64 * v + c, 8, stride=8), :] = first[c]
                t_local[pl.ds(192 + 64 * v + c, 8, stride=8), :] = second[c]
        for which in range(2):
            for j in range(LOCAL_ROWS):
                start = 8 * (which * 24 + j)
                split_rows(t_local[start : start + 8, :], lhs_local, which * LOCAL_ROWS + j)
        return scatter(lhs_local, one_hot)

    def rim_values(k, index_ref, v):
        index = index_ref[8 * v : 8 * v + 8, :]
        fine, upper = index % 128, index >= 128
        out = []
        for pair in range(3):
            got = []
            for c in (2 * pair, 2 * pair + 1):
                halves = [lanes(splat(field[k, 8 * c + t : 8 * c + t + 1, :]), fine) for t in range(2)]
                got.append(jnp.where(upper, halves[1], halves[0]))
            out.append(jnp.where(lane < 64, got[0], got[1]))
        return out

    def own_values(k):
        for v in range(4):
            got = rim_values(k, rim_idx, v)
            for pair in range(3):
                mine[pair, 8 * v : 8 * v + 8, :] = got[pair]

    def send_values(k):
        for v in range(4):
            got = rim_values(k, rim_out, v)
            for pair in range(3):
                send_v[k - 1, 8 * v : 8 * v + 8, pair, :] = got[pair]
        copies = []
        for side in farthest_first:
            copy = pltpu.make_async_remote_copy(
                src_ref=send_v.at[k - 1, side + 2],
                dst_ref=recv_v.at[k - 1, 27 - side],
                send_sem=v_send.at[k - 1, side],
                recv_sem=v_recv.at[k - 1, 25 - side],
                device_id=near[side],
                device_id_type=MESH,
            )
            copy.start()
            copies.append(copy)
        own_values(k)
        return copies

    def rim_contacts(k):
        work = jnp.zeros((8, 128), F32)
        for v in range(4):
            rows = slice(8 * v, 8 * v + 8)
            a, b = [], []
            for pair in range(3):
                own = mine[pair, rows, :]
                a += [own, pltpu.roll(own, 64, 1)]
                if k > 0:
                    got = recv_v[k - 1, rows, pair, :]
                    b += [got, pltpu.roll(got, 64, 1)]
                else:
                    far = rim_far[rows, :]
                    for c in (2 * pair, 2 * pair + 1):
                        halves = [lanes(recv_q[rows, 2 * c + t, :], far % 128) for t in range(2)]
                        b.append(jnp.where(far >= 128, halves[1], halves[0]))
            first, done = response(
                a, b,
                [rim_geo[c, rows, :] for c in range(3)],
                rim_geo[3, rows, :], rim_geo[4, rows, :],
                [rim_geo[5 + q, rows, :] for q in range(4)], False,
            )
            for c in range(6):
                t_rim[pl.ds(64 * v + c, 8, stride=8), :] = first[c]
            work = work + done
        return jnp.sum(jnp.where(lane >= 32, work, 0.0), keepdims=True)

    def rim_forces():
        for i in range(SIDES // 2):
            start = 16 * (i + 1)
            even, odd = t_rim[start : start + 8, :], t_rim[start + 8 : start + 16, :]
            split_rows(jnp.where(lane < 64, even, pltpu.roll(odd, 64, 1)), lhs_rim, i)
        return scatter(lhs_rim, rim_hot)

    sums = []

    def total_of(x):
        folded = x[0:8]
        for t in range(1, 6):
            folded = folded + x[8 * t : 8 * t + 8]
        return jnp.sum(folded, keepdims=True)

    lane_row = lane[0:1]

    def pack(values):
        out = jnp.zeros((1, 128), F32)
        for j, value in enumerate(values):
            out = jnp.where(lane_row == j, value, out)
        return out

    def spread(stage, where, buffer, rank, value):
        row_buf[stage] = value
        buffer[rank] = value
        copies = []
        for j, device in enumerate(where):
            copy = pltpu.make_async_remote_copy(
                src_ref=row_buf.at[stage],
                dst_ref=buffer.at[rank],
                send_sem=s_send.at[stage, j],
                recv_sem=s_recv.at[stage, j],
                device_id=device,
                device_id_type=MESH,
            )
            copy.start()
            copies.append(copy)
        return copies

    def gather_sum(copies, buffer, count):
        for copy in copies:
            copy.wait_recv()
        level = [buffer[j] for j in range(count)]
        while len(level) > 1:
            level = [level[j] + level[j + 1] for j in range(0, len(level), 2)]
        return level[0]

    def lane_of(values, j):
        return jnp.sum(jnp.where(lane_row == j, values, 0.0), keepdims=True)

    def meet():
        for v in range(4):
            rows = slice(8 * v, 8 * v + 8)
            seg = [rim_geo[q, rows, :] for q in range(8)]
            got = [recv_q[rows, 12 + h, :] for h in range(2)]

            def theirs(h, p):
                return lanes(got[h], lane % 32 + 32 * p)

            ours = lane % 64 >= 32
            valid = (lane < 64) & (row + 8 * v >= 2) & (row + 8 * v < 28)
            index = jnp.where(ours, seg[0], theirs(0, 0))
            kind = jnp.where(ours, seg[2], theirs(0, 1))
            rim_idx[rows, :] = index.astype(jnp.int32)
            flipped = jnp.where(ours, theirs(0, 0), seg[0])
            rim_out[rows, :] = flipped.astype(jnp.int32)
            rim_far[rows, :] = jnp.where(ours, seg[1], theirs(1, 3)).astype(jnp.int32)
            for c in range(3):
                rim_geo[c, rows, :] = jnp.where(ours, seg[3 + c], -theirs(1, c))
            rim_geo[3, rows, :] = jnp.where(ours, seg[6], theirs(0, 3))
            rim_geo[4, rows, :] = jnp.where(ours, seg[7], theirs(0, 2))
            coeff = coefficients(kind, valid)
            for q in range(4):
                rim_geo[5 + q, rows, :] = coeff[q]
        own_values(0)
        turned = jnp.transpose(jnp.concatenate([rim_idx[...].astype(F32), rim_pad], axis=0))
        rim_rows(turned, 0, 0)

    sent = list(q_copies)

    def tile(ref, t):
        return ref[pl.ds(t, 8, stride=8), :]

    def product(k, t, forces):
        return tile(diag, t) * tile(field.at[k], t) - forces

    def apply(k, copies, finish, between=None):
        whole = local_forces(k)
        if between is not None:
            between()
        for t in range(2, 8):
            field[k + 1, pl.ds(t, 8, stride=8), :] = finish(product(k, t, whole[:, 128 * t : 128 * (t + 1)]), t)
        start = [product(k, t, whole[:, 128 * t : 128 * (t + 1)]) for t in range(2)]
        for copy in copies:
            copy.wait_recv()
        if k == 0:
            meet()
        rim_contacts(k)
        rim = rim_forces()
        for t in range(2):
            value = start[t] - rim[:, 128 * t : 128 * (t + 1)]
            field[k + 1, pl.ds(t, 8, stride=8), :] = finish(value, t)
        out = send_values(k + 1)
        sent.extend(out)
        return out

    def plain(value, t):
        return value

    def dense_of(k):
        return field[k, 0:48, :]

    w0 = dense_of(0)
    copies = apply(0, q_copies, plain)
    w1 = dense_of(1)
    first_sums = pack([total_of(w0 * w0), total_of(w0 * w1), total_of(w1 * w1)])
    early = spread(0, plane, plane_buf.at[0], plane_rank, first_sums)
    sent += early
    held = {}

    def onward():
        held["line"] = spread(1, line, line_buf.at[0], line_rank, gather_sum(early, plane_buf.at[0], PLANE))
        sent.extend(held["line"])

    copies = apply(1, copies, plain, onward)

    def settle():
        total = gather_sum(held["line"], line_buf.at[0], LINE)
        m0, m1, m2 = lane_of(total, 0), lane_of(total, 1), lane_of(total, 2)
        held["inv"] = jnp.sqrt(m0 / m2)
        held["shift"] = m1 / m0 * held["inv"]

    def centred(value, t):
        inv, shift = held["inv"], held["shift"]
        inv2 = inv * inv
        b, p, q = [tile(field.at[j], t) for j in range(3)]
        p, q = p * inv, q * inv2
        return value * (inv2 * inv) - shift * (3.0 * q - shift * (3.0 * p - shift * b))

    copies = apply(2, copies, centred, settle)
    inv, shift = held["inv"], held["shift"]
    u0, u3 = w0, dense_of(3)
    p, q = w1 * inv, dense_of(2) * (inv * inv)
    u1 = p - shift * u0
    u2 = q - shift * (2.0 * p - shift * u0)
    basis = [u0, u1, u2, u3]
    pairs = [(0, 0), (0, 1), (1, 1), (1, 2), (2, 2), (2, 3), (3, 3)]
    known = [total_of(basis[i] * basis[j]) for i, j in pairs]
    whole = local_forces(3)
    near_work = jnp.zeros((8, 128), F32)
    for t in range(8):
        value = product(3, t, whole[:, 128 * t : 128 * (t + 1)])
        field[4, pl.ds(t, 8, stride=8), :] = value
        near_work = near_work + value * tile(field.at[3], t)
    near_work = inv * jnp.sum(near_work, keepdims=True) - shift * known[6]
    for copy in copies:
        copy.wait_recv()
    last = near_work + inv * rim_contacts(3)
    late = spread(2, plane, plane_buf.at[1], plane_rank, pack(known + [last]))
    sent += late
    rim = rim_forces()
    for t in range(2):
        value = tile(field.at[4], t) - rim[:, 128 * t : 128 * (t + 1)]
        field[4, pl.ds(t, 8, stride=8), :] = value
    u4 = dense_of(4) * inv - shift * u3
    late = spread(3, line, line_buf.at[1], line_rank, gather_sum(late, plane_buf.at[1], PLANE))
    sent += late
    sums = gather_sum(late, line_buf.at[1], LINE)
    mu = [lane_of(sums, j) for j in range(8)]

    scale = 1.0 / inv

    def inner(p, q):
        by_degree = {}
        for i, x in enumerate(p):
            for j, y in enumerate(q):
                term = x * y
                by_degree[i + j] = by_degree[i + j] + term if i + j in by_degree else term
        out = None
        for degree, term in by_degree.items():
            term = term * mu[degree]
            out = term if out is None else out + term
        return out

    one = jnp.ones((1, 1), F32)
    res, direction, answer = [one], [one], []
    norm = mu[0]
    for step in range(4):
        image = [shift * direction[0]]
        for i in range(1, len(direction)):
            image.append(direction[i - 1] + shift * direction[i])
        image.append(direction[-1])
        image = [scale * value for value in image]
        alpha = norm / inner(direction, image)
        answer = [
            alpha * direction[i] + (answer[i] if i < len(answer) else 0.0)
            for i in range(len(direction))
        ]
        res = [
            (res[i] if i < len(res) else 0.0) - alpha * image[i]
            for i in range(len(image))
        ]
        if step < 3:
            fresh = inner(res, res)
            ratio = fresh / norm
            direction = [
                res[i] + (ratio * direction[i] if i < len(direction) else 0.0)
                for i in range(len(res))
            ]
            norm = fresh
    basis.append(u4)
    x = answer[0] * basis[0]
    for i in range(1, 4):
        x = x + answer[i] * basis[i]
    r = res[0] * basis[0]
    for i in range(1, 5):
        r = r + res[i] * basis[i]
    x_ref[0:48] = x
    x_ref[48:96] = r
    for copy in sent:
        copy.wait_send()


def shards(*arguments):
    arguments = [
        x if x.ndim == 2 or x.shape[3] == 2 else x.reshape(x.size // 128, 128) for x in arguments
    ]
    vmem = pl.BlockSpec(memory_space=pltpu.VMEM)
    hbm = pl.BlockSpec(memory_space=pltpu.HBM)
    out = jax.ShapeDtypeStruct((48, 128), F32)
    dma = pltpu.SemaphoreType.DMA
    outs = pl.pallas_call(
        kernel,
        out_shape=pltpu.VMEM((96, 128), F32),
        in_specs=[hbm] * 8,
        out_specs=vmem,
        scratch_shapes=[
            pltpu.VMEM((48, 128), F32),
            pltpu.VMEM((48, 128), F32),
            pltpu.VMEM((4, 4), F32),
            pltpu.VMEM((24, 128), jnp.int32),
            pltpu.VMEM((24, 128), jnp.int32),
            pltpu.VMEM((24, 128), jnp.int32),
            pltpu.VMEM((72, 128), F32),
            pltpu.VMEM((2, 3072), F32),
            pltpu.VMEM((8, 24, 128), F32),
            pltpu.VMEM((24, 128), jnp.int32),
            pltpu.VMEM((24, 128), jnp.int32),
            pltpu.VMEM((4, 24, 128), F32),
            pltpu.VMEM((2 * LOCAL_ROWS * 128, GRAINS), BF16),
            pltpu.VMEM((2 * 24 * 8, 128), F32),
            pltpu.VMEM((32, 2 * LOCAL_ROWS * 128), BF16),
            pltpu.VMEM((32, 128), jnp.int32),
            pltpu.VMEM((32, 128), jnp.int32),
            pltpu.VMEM((32, 128), jnp.int32),
            pltpu.VMEM((9, 32, 128), F32),
            pltpu.VMEM((SIDES * 64, RIM), BF16),
            pltpu.VMEM((32 * 8, 128), F32),
            pltpu.VMEM((32, SIDES * 64), BF16),
            pltpu.VMEM((5, 64, 128), F32),
            pltpu.VMEM((64, 128), F32),
            pltpu.VMEM((3, 32, 128), F32),
            pltpu.VMEM((32, 14, 128), F32),
            pltpu.VMEM((32, 14, 128), F32),
            pltpu.VMEM((3, 32, 3, 128), F32),
            pltpu.VMEM((3, 32, 3, 128), F32),
            pltpu.VMEM((4, 1, 128), F32),
            pltpu.VMEM((2, PLANE, 1, 128), F32),
            pltpu.VMEM((2, LINE, 1, 128), F32),
            dma((8,)),
            dma((SIDES,)),
            dma((SIDES,)),
            dma((3, SIDES)),
            dma((3, SIDES)),
            dma((4, PLANE)),
            dma((4, PLANE)),
        ],
        compiler_params=pltpu.CompilerParams(
            collective_id=0, has_side_effects=True, vmem_limit_bytes=56 * 1024 * 1024
        ),
    )(*arguments)
    return tuple(outs[48*i:48*i+48].reshape(1, 1, 1, 6, GRAINS) for i in range(2))


def solution(mesh):
    placed = P("gx", "gy", "gz", None, None)
    flat = P("gx", "gy", "gz", None)
    return jax.shard_map(
        shards,
        mesh=mesh,
        in_specs=(placed, placed, P(), flat, flat, flat, placed, placed),
        out_specs=(placed, placed),
        check_vma=False,
    )
```

```python
import functools

import jax
import jax.numpy as jnp
from jax import lax
from jax.experimental import pallas as pl
from jax.experimental.pallas import tpu as pltpu
from jax.sharding import PartitionSpec as P

F32 = jnp.float32
BF16 = jnp.bfloat16
MESH = pl.DeviceIdType.MESH
GRAINS = 1024
RIM = 256
NEAR = 2240
TYPES = 4
SIDES = 26
LOCAL_ROWS = 18
NX, NY, NZ = 4, 8, 16
ZLO = 4
PLANE = 32
LINE = 16


def offset_of(side):
    whole = side + (1 if side >= 13 else 0)
    return (whole // 9 - 1, whole // 3 % 3 - 1, whole % 3 - 1)


def cross(w, n):
    return [
        w[1] * n[2] - w[2] * n[1],
        w[2] * n[0] - w[0] * n[2],
        w[0] * n[1] - w[1] * n[0],
    ]


def response(a, b, n, ra, rb, coeff, both):
    shear, normal_less, roll, twist_less = coeff
    arm = [rb * b[3 + c] + ra * a[3 + c] for c in range(3)]
    turn = cross(arm, n)
    delta = [b[c] - a[c] - turn[c] for c in range(3)]
    along = normal_less * (n[0] * delta[0] + n[1] * delta[1] + n[2] * delta[2])
    force = [shear * delta[c] + along * n[c] for c in range(3)]
    theta = [b[3 + c] - a[3 + c] for c in range(3)]
    twist = twist_less * (n[0] * theta[0] + n[1] * theta[1] + n[2] * theta[2])
    moment = [roll * theta[c] + twist * n[c] for c in range(3)]
    lever = cross(n, force)
    first = force + [ra * lever[c] + moment[c] for c in range(3)]
    if not both:
        work = [force[c] * delta[c] + moment[c] * theta[c] for c in range(3)]
        return first, work[0] + work[1] + work[2]
    second = [-f for f in force] + [rb * lever[c] - moment[c] for c in range(3)]
    return first, second


def lanes(x, index):
    return jnp.take_along_axis(x, index, axis=1, mode="promise_in_bounds")


def splat(row):
    return jnp.broadcast_to(row, (8, 128))


def kernel(
    rhs_in, diag_in, stiff_in, own_in, slot_in, type_in, normal_in, radii_in,
    x_ref,
    rhs_ref, diag_ref, stiff_ref, own_ref, slot_ref, type_ref, normal_ref, radii_ref,
    dense, idx_a, idx_b, geo, one_hot, t_local, lhs_local,
    rim_idx, rim_far, rim_out, rim_geo, rim_hot, t_rim, lhs_rim, field, diag, mine,
    send_q, recv_q, send_v, recv_v, row_buf, plane_buf, line_buf,
    in_sem, q_send, q_recv, v_send, v_recv, s_send, s_recv,
):
    loads = []
    for j, (source, target) in enumerate((
        (rhs_in, rhs_ref), (own_in, own_ref), (slot_in, slot_ref), (type_in, type_ref),
        (normal_in, normal_ref), (radii_in.at[0, 0, 0], radii_ref), (stiff_in, stiff_ref),
        (diag_in, diag_ref),
    )):
        load = pltpu.make_async_copy(source, target, in_sem.at[j])
        load.start()
        loads.append(load)
    gx, gy, gz = lax.axis_index("gx"), lax.axis_index("gy"), lax.axis_index("gz")
    wide, low = gz // ZLO, gz % ZLO

    def distance(side):
        dx, dy, dz = offset_of(side)
        return (dx == 0, dx * dz >= 0, -abs(dz), -abs(dy))

    farthest_first = sorted(range(SIDES), key=distance)
    near = []
    for side in range(SIDES):
        dx, dy, dz = offset_of(side)
        near.append(((gx + (dx + NX)) % NX, (gy + (dy + NY)) % NY, (gz + (dz + NZ)) % NZ))
    plane = []
    for j in range(1, PLANE):
        dy, dw = j // ZLO, j % ZLO
        plane.append((gx, (gy + dy) % NY, ((wide + dw) % ZLO) * ZLO + low))
    line = []
    for j in range(1, LINE):
        dx, dl = j // ZLO, j % ZLO
        line.append(((gx + dx) % NX, gy, wide * ZLO + (low + dl) % ZLO))
    plane_rank = gy * ZLO + wide
    line_rank = gx * ZLO + low

    lane = lax.broadcasted_iota(jnp.int32, (8, 128), 1)
    row = lax.broadcasted_iota(jnp.int32, (8, 128), 0)

    barrier = pltpu.get_barrier_semaphore()
    for where in near + plane + line:
        pl.semaphore_signal(barrier, inc=1, device_id=where, device_id_type=MESH)

    recv_q[0:2] = jnp.zeros((2, 14, 128), F32)
    recv_q[28:32] = jnp.zeros((4, 14, 128), F32)
    for e in range(3):
        recv_v[e, 0:2] = jnp.zeros((2, 3, 128), F32)
        recv_v[e, 28:32] = jnp.zeros((4, 3, 128), F32)

    for load in loads:
        load.wait()

    dense[0] = own_ref[...].astype(F32)
    dense[1] = slot_ref[...].astype(F32)
    dense[2] = type_ref[...].astype(F32)
    for c in range(3):
        dense[3 + c] = normal_ref[24 * c : 24 * c + 24, :]
    for c in range(2):
        for i in range(24):
            dense[6 + c, i : i + 1, :] = radii_ref[c : c + 1, 128 * i : 128 * (i + 1)]

    stiffness = [
        [jnp.broadcast_to(stiff_ref[q : q + 1, t : t + 1], (8, 128)) for t in range(TYPES)]
        for q in range(4)
    ]

    def coefficients(kind, valid):
        out = []
        for q in range(4):
            total = jnp.zeros_like(kind)
            for t in range(TYPES):
                total = jnp.where(kind == float(t), stiffness[q][t], total)
            out.append(jnp.where(valid, total, 0.0))
        return [out[1], out[0] - out[1], out[2], out[3] - out[2]]

    def segments(q, v):
        low_row = dense[q, 17 + 2 * v : 18 + 2 * v, :]
        nxt = min(18 + 2 * v, 23)
        high_row = dense[q, nxt : nxt + 1, :]
        base = jnp.where(row < 4, splat(low_row), splat(high_row))
        return lanes(base, (lane % 32) + 32 * (row % 4))

    def quarter(parts):
        out = parts[3]
        for p in (2, 1, 0):
            out = jnp.where(lane < 32 * (p + 1), parts[p], out)
        return out

    kept = []
    for v in range(4):
        seg = [segments(q, v) for q in range(8)]
        side = (row + (8 * v - 2)).astype(F32)
        slot_rim = seg[1] - (GRAINS + RIM * side)
        rows = slice(8 * v, 8 * v + 8)
        send_q[rows, 12, :] = quarter([slot_rim, seg[2], seg[6], seg[7]])
        send_q[rows, 13, :] = quarter([seg[3], seg[4], seg[5], seg[0]])
        seg[1] = slot_rim
        kept.append(seg)
    for v in range(4):
        for q in range(8):
            rim_geo[q, 8 * v : 8 * v + 8, :] = kept[v][q]
    rim = jnp.concatenate([rhs_ref[8 * c : 8 * c + 2, :] for c in range(6)], axis=0)
    for side in range(SIDES):
        send_q[side + 2, 0:12, :] = rim

    pl.semaphore_wait(barrier, SIDES + PLANE - 1 + LINE - 1)

    def exchange(source, target, send_sem, recv_sem):
        for side in farthest_first:
            pltpu.make_async_remote_copy(
                src_ref=source.at[side + 2],
                dst_ref=target.at[27 - side],
                send_sem=send_sem,
                recv_sem=recv_sem,
                device_id=near[side],
                device_id_type=MESH,
            ).start()
        return pltpu.make_async_remote_copy(
            src_ref=source.at[2:28],
            dst_ref=target.at[2:28],
            send_sem=send_sem,
            recv_sem=recv_sem,
            device_id=near[0],
            device_id_type=MESH,
        )

    arriving = exchange(send_q, recv_q, q_send.at[0], q_recv.at[0])

    for v in range(3):
        rows = slice(8 * v, 8 * v + 8)
        number = (row + 8 * v) * 128 + lane
        inside = number < NEAR
        own = dense[0, rows, :]
        slot = jnp.where(inside, dense[1, rows, :], 0.0)
        idx_a[rows, :] = own.astype(jnp.int32)
        idx_b[rows, :] = slot.astype(jnp.int32)
        dense[1, rows, :] = slot
        coeff = coefficients(dense[2, rows, :], inside)
        for q in range(4):
            geo[q, rows, :] = coeff[q]

    column = lax.broadcasted_iota(jnp.int32, (128, 128), 1).astype(F32)
    pad = jnp.zeros((128 - 24, 128), F32)
    for which in range(2):
        turned = jnp.transpose(jnp.concatenate([dense[which], pad], axis=0))
        for j in range(LOCAL_ROWS):
            spread = jnp.broadcast_to(turned[:, j : j + 1], (128, 128))
            at = (which * LOCAL_ROWS + j) * 128
            for g in range(8):
                hit = jnp.where(spread == column + float(128 * g), 1.0, 0.0)
                one_hot[at : at + 128, 128 * g : 128 * (g + 1)] = hit.astype(BF16)

    def rim_rows(turned, first_row, at):
        for i in range(SIDES):
            spread_idx = jnp.broadcast_to(turned[first_row : first_row + 32, i + 2 : i + 3], (32, 128))
            start = 64 * i + at
            for g in range(2):
                hit = jnp.where(spread_idx == column[0:32] + float(128 * g), 1.0, 0.0)
                rim_hot[start : start + 32, 128 * g : 128 * (g + 1)] = hit.astype(BF16)

    rim_pad = jnp.zeros((96, 128), F32)
    rim_rows(jnp.transpose(jnp.concatenate([rim_geo[0], rim_pad], axis=0)), 0, 32)

    t_local[...] = jnp.zeros_like(t_local)
    t_rim[...] = jnp.zeros_like(t_rim)
    lhs_local[...] = jnp.zeros_like(lhs_local)
    lhs_rim[...] = jnp.zeros_like(lhs_rim)

    field[0, 0:48, :] = rhs_ref[...]
    field[0, 48:64, :] = jnp.zeros((16, 128), F32)
    diag[0:48, :] = diag_ref[...]
    diag[48:64, :] = jnp.zeros((16, 128), F32)

    def split_rows(whole, target, at):
        high = whole.astype(BF16).astype(F32)
        rest = whole - high
        mid = rest.astype(BF16).astype(F32)
        low_part = rest - mid
        cut = slice(128 * at, 128 * (at + 1))
        target[0:16, cut] = jnp.concatenate([high, mid], axis=0).astype(BF16)
        target[16:32, cut] = jnp.concatenate([low_part, jnp.zeros_like(low_part)], axis=0).astype(BF16)

    def scatter(lhs, hot):
        out = jnp.dot(lhs[...], hot[...], preferred_element_type=F32)
        return out[0:8] + out[8:16] + out[16:24]

    def local_forces(k):
        for v in range(3):
            rows = slice(8 * v, 8 * v + 8)
            ends = []
            for index_ref in (idx_a, idx_b):
                index = index_ref[rows, :]
                fine, coarse = index % 128, index // 128
                hits = [coarse == t for t in range(1, 8)]
                got = []
                for c in range(6):
                    total = lanes(splat(field[k, 8 * c : 8 * c + 1, :]), fine)
                    for t in range(1, 8):
                        table = splat(field[k, 8 * c + t : 8 * c + t + 1, :])
                        total = jnp.where(hits[t - 1], lanes(table, fine), total)
                    got.append(total)
                ends.append(got)
            first, second = response(
                ends[0], ends[1],
                [dense[3 + c, rows, :] for c in range(3)],
                dense[6, rows, :], dense[7, rows, :],
                [geo[q, rows, :] for q in range(4)], True,
            )
            for c in range(6):
                t_local[pl.ds(64 * v + c, 8, stride=8), :] = first[c]
                t_local[pl.ds(192 + 64 * v + c, 8, stride=8), :] = second[c]
        for which in range(2):
            for j in range(LOCAL_ROWS):
                start = 8 * (which * 24 + j)
                split_rows(t_local[start : start + 8, :], lhs_local, which * LOCAL_ROWS + j)
        return scatter(lhs_local, one_hot)

    def rim_values(k, index_ref, v):
        index = index_ref[8 * v : 8 * v + 8, :]
        fine, upper = index % 128, index >= 128
        out = []
        for pair in range(3):
            got = []
            for c in (2 * pair, 2 * pair + 1):
                halves = [lanes(splat(field[k, 8 * c + t : 8 * c + t + 1, :]), fine) for t in range(2)]
                got.append(jnp.where(upper, halves[1], halves[0]))
            out.append(jnp.where(lane < 64, got[0], got[1]))
        return out

    def own_values(k):
        for v in range(4):
            got = rim_values(k, rim_idx, v)
            for pair in range(3):
                mine[pair, 8 * v : 8 * v + 8, :] = got[pair]

    def send_values(k):
        for v in range(4):
            got = rim_values(k, rim_out, v)
            for pair in range(3):
                send_v[k - 1, 8 * v : 8 * v + 8, pair, :] = got[pair]
        out = exchange(send_v.at[k - 1], recv_v.at[k - 1], v_send.at[k - 1], v_recv.at[k - 1])
        own_values(k)
        return out

    def rim_contacts(k):
        work = jnp.zeros((8, 128), F32)
        for v in range(4):
            rows = slice(8 * v, 8 * v + 8)
            a, b = [], []
            for pair in range(3):
                own = mine[pair, rows, :]
                a += [own, pltpu.roll(own, 64, 1)]
                if k > 0:
                    got = recv_v[k - 1, rows, pair, :]
                    b += [got, pltpu.roll(got, 64, 1)]
                else:
                    far = rim_far[rows, :]
                    for c in (2 * pair, 2 * pair + 1):
                        halves = [lanes(recv_q[rows, 2 * c + t, :], far % 128) for t in range(2)]
                        b.append(jnp.where(far >= 128, halves[1], halves[0]))
            first, done = response(
                a, b,
                [rim_geo[c, rows, :] for c in range(3)],
                rim_geo[3, rows, :], rim_geo[4, rows, :],
                [rim_geo[5 + q, rows, :] for q in range(4)], False,
            )
            for c in range(6):
                t_rim[pl.ds(64 * v + c, 8, stride=8), :] = first[c]
            work = work + done
        return jnp.sum(jnp.where(lane >= 32, work, 0.0), keepdims=True)

    def rim_forces():
        for i in range(SIDES // 2):
            start = 16 * (i + 1)
            even, odd = t_rim[start : start + 8, :], t_rim[start + 8 : start + 16, :]
            split_rows(jnp.where(lane < 64, even, pltpu.roll(odd, 64, 1)), lhs_rim, i)
        return scatter(lhs_rim, rim_hot)

    sums = []

    def total_of(x):
        folded = x[0:8]
        for t in range(1, 6):
            folded = folded + x[8 * t : 8 * t + 8]
        return jnp.sum(folded, keepdims=True)

    lane_row = lane[0:1]

    def pack(values):
        out = jnp.zeros((1, 128), F32)
        for j, value in enumerate(values):
            out = jnp.where(lane_row == j, value, out)
        return out

    def spread(stage, where, buffer, rank, value):
        row_buf[stage] = value
        buffer[rank] = value
        for device in where:
            pltpu.make_async_remote_copy(
                src_ref=row_buf.at[stage],
                dst_ref=buffer.at[rank],
                send_sem=s_send.at[stage],
                recv_sem=s_recv.at[stage],
                device_id=device,
                device_id_type=MESH,
            ).start()
        count = len(where)
        return pltpu.make_async_remote_copy(
            src_ref=buffer.at[0:count],
            dst_ref=buffer.at[0:count],
            send_sem=s_send.at[stage],
            recv_sem=s_recv.at[stage],
            device_id=where[0],
            device_id_type=MESH,
        )

    def gather_sum(arriving, buffer, count):
        arriving.wait_recv()
        level = [buffer[j] for j in range(count)]
        while len(level) > 1:
            level = [level[j] + level[j + 1] for j in range(0, len(level), 2)]
        return level[0]

    def lane_of(values, j):
        return jnp.sum(jnp.where(lane_row == j, values, 0.0), keepdims=True)

    def meet():
        for v in range(4):
            rows = slice(8 * v, 8 * v + 8)
            seg = [rim_geo[q, rows, :] for q in range(8)]
            got = [recv_q[rows, 12 + h, :] for h in range(2)]

            def theirs(h, p):
                return lanes(got[h], lane % 32 + 32 * p)

            ours = lane % 64 >= 32
            valid = (lane < 64) & (row + 8 * v >= 2) & (row + 8 * v < 28)
            index = jnp.where(ours, seg[0], theirs(0, 0))
            kind = jnp.where(ours, seg[2], theirs(0, 1))
            rim_idx[rows, :] = index.astype(jnp.int32)
            flipped = jnp.where(ours, theirs(0, 0), seg[0])
            rim_out[rows, :] = flipped.astype(jnp.int32)
            rim_far[rows, :] = jnp.where(ours, seg[1], theirs(1, 3)).astype(jnp.int32)
            for c in range(3):
                rim_geo[c, rows, :] = jnp.where(ours, seg[3 + c], -theirs(1, c))
            rim_geo[3, rows, :] = jnp.where(ours, seg[6], theirs(0, 3))
            rim_geo[4, rows, :] = jnp.where(ours, seg[7], theirs(0, 2))
            coeff = coefficients(kind, valid)
            for q in range(4):
                rim_geo[5 + q, rows, :] = coeff[q]
        own_values(0)
        turned = jnp.transpose(jnp.concatenate([rim_idx[...].astype(F32), rim_pad], axis=0))
        rim_rows(turned, 0, 0)

    sent = [arriving]

    def tile(ref, t):
        return ref[pl.ds(t, 8, stride=8), :]

    def product(k, t, forces):
        return tile(diag, t) * tile(field.at[k], t) - forces

    def apply(k, arriving, finish, between=None):
        whole = local_forces(k)
        if between is not None:
            between()
        for t in range(2, 8):
            field[k + 1, pl.ds(t, 8, stride=8), :] = finish(product(k, t, whole[:, 128 * t : 128 * (t + 1)]), t)
        start = [product(k, t, whole[:, 128 * t : 128 * (t + 1)]) for t in range(2)]
        arriving.wait_recv()
        if k == 0:
            meet()
        rim_contacts(k)
        rim = rim_forces()
        for t in range(2):
            value = start[t] - rim[:, 128 * t : 128 * (t + 1)]
            field[k + 1, pl.ds(t, 8, stride=8), :] = finish(value, t)
        out = send_values(k + 1)
        sent.append(out)
        return out

    def plain(value, t):
        return value

    def dense_of(k):
        return field[k, 0:48, :]

    w0 = dense_of(0)
    arriving = apply(0, arriving, plain)
    w1 = dense_of(1)
    first_sums = pack([total_of(w0 * w0), total_of(w0 * w1), total_of(w1 * w1)])
    early = spread(0, plane, plane_buf.at[0], plane_rank, first_sums)
    sent.append(early)
    held = {}

    def onward():
        held["line"] = spread(1, line, line_buf.at[0], line_rank, gather_sum(early, plane_buf.at[0], PLANE))
        sent.append(held["line"])

    arriving = apply(1, arriving, plain, onward)

    def settle():
        total = gather_sum(held["line"], line_buf.at[0], LINE)
        m0, m1, m2 = lane_of(total, 0), lane_of(total, 1), lane_of(total, 2)
        held["inv"] = jnp.sqrt(m0 / m2)
        held["shift"] = m1 / m0 * held["inv"]

    def centred(value, t):
        inv, shift = held["inv"], held["shift"]
        inv2 = inv * inv
        b, p, q = [tile(field.at[j], t) for j in range(3)]
        p, q = p * inv, q * inv2
        return value * (inv2 * inv) - shift * (3.0 * q - shift * (3.0 * p - shift * b))

    arriving = apply(2, arriving, centred, settle)
    inv, shift = held["inv"], held["shift"]
    u0, u3 = w0, dense_of(3)
    p, q = w1 * inv, dense_of(2) * (inv * inv)
    u1 = p - shift * u0
    u2 = q - shift * (2.0 * p - shift * u0)
    basis = [u0, u1, u2, u3]
    pairs = [(0, 0), (0, 1), (1, 1), (1, 2), (2, 2), (2, 3), (3, 3)]
    known = [total_of(basis[i] * basis[j]) for i, j in pairs]
    whole = local_forces(3)
    near_work = jnp.zeros((8, 128), F32)
    for t in range(8):
        value = product(3, t, whole[:, 128 * t : 128 * (t + 1)])
        field[4, pl.ds(t, 8, stride=8), :] = value
        near_work = near_work + value * tile(field.at[3], t)
    near_work = inv * jnp.sum(near_work, keepdims=True) - shift * known[6]
    arriving.wait_recv()
    last = near_work + inv * rim_contacts(3)
    late = spread(2, plane, plane_buf.at[1], plane_rank, pack(known + [last]))
    rim = rim_forces()
    for t in range(2):
        value = tile(field.at[4], t) - rim[:, 128 * t : 128 * (t + 1)]
        field[4, pl.ds(t, 8, stride=8), :] = value
    u4 = dense_of(4) * inv - shift * u3
    for done in sent:
        done.wait_send()
    sums = gather_sum(late, plane_buf.at[1], PLANE)
    late.wait_send()
    late = spread(3, line, line_buf.at[1], line_rank, sums)
    sums = gather_sum(late, line_buf.at[1], LINE)
    late.wait_send()
    mu = [lane_of(sums, j) for j in range(8)]

    scale = 1.0 / inv

    def inner(p, q):
        by_degree = {}
        for i, x in enumerate(p):
            for j, y in enumerate(q):
                term = x * y
                by_degree[i + j] = by_degree[i + j] + term if i + j in by_degree else term
        out = None
        for degree, term in by_degree.items():
            term = term * mu[degree]
            out = term if out is None else out + term
        return out

    one = jnp.ones((1, 1), F32)
    res, direction, answer = [one], [one], []
    norm = mu[0]
    for step in range(4):
        image = [shift * direction[0]]
        for i in range(1, len(direction)):
            image.append(direction[i - 1] + shift * direction[i])
        image.append(direction[-1])
        image = [scale * value for value in image]
        alpha = norm / inner(direction, image)
        answer = [
            alpha * direction[i] + (answer[i] if i < len(answer) else 0.0)
            for i in range(len(direction))
        ]
        res = [
            (res[i] if i < len(res) else 0.0) - alpha * image[i]
            for i in range(len(image))
        ]
        if step < 3:
            fresh = inner(res, res)
            ratio = fresh / norm
            direction = [
                res[i] + (ratio * direction[i] if i < len(direction) else 0.0)
                for i in range(len(res))
            ]
            norm = fresh
    basis.append(u4)
    x = answer[0] * basis[0]
    for i in range(1, 4):
        x = x + answer[i] * basis[i]
    r = res[0] * basis[0]
    for i in range(1, 5):
        r = r + res[i] * basis[i]
    x_ref[0:48] = x
    x_ref[48:96] = r


def shards(*arguments):
    arguments = [
        x if x.ndim == 2 or x.shape[3] == 2 else x.reshape(x.size // 128, 128) for x in arguments
    ]
    vmem = pl.BlockSpec(memory_space=pltpu.VMEM)
    hbm = pl.BlockSpec(memory_space=pltpu.HBM)
    out = jax.ShapeDtypeStruct((48, 128), F32)
    dma = pltpu.SemaphoreType.DMA
    outs = pl.pallas_call(
        kernel,
        out_shape=pltpu.VMEM((96, 128), F32),
        in_specs=[hbm] * 8,
        out_specs=vmem,
        scratch_shapes=[
            pltpu.VMEM((48, 128), F32),
            pltpu.VMEM((48, 128), F32),
            pltpu.VMEM((4, 4), F32),
            pltpu.VMEM((24, 128), jnp.int32),
            pltpu.VMEM((24, 128), jnp.int32),
            pltpu.VMEM((24, 128), jnp.int32),
            pltpu.VMEM((72, 128), F32),
            pltpu.VMEM((2, 3072), F32),
            pltpu.VMEM((8, 24, 128), F32),
            pltpu.VMEM((24, 128), jnp.int32),
            pltpu.VMEM((24, 128), jnp.int32),
            pltpu.VMEM((4, 24, 128), F32),
            pltpu.VMEM((2 * LOCAL_ROWS * 128, GRAINS), BF16),
            pltpu.VMEM((2 * 24 * 8, 128), F32),
            pltpu.VMEM((32, 2 * LOCAL_ROWS * 128), BF16),
            pltpu.VMEM((32, 128), jnp.int32),
            pltpu.VMEM((32, 128), jnp.int32),
            pltpu.VMEM((32, 128), jnp.int32),
            pltpu.VMEM((9, 32, 128), F32),
            pltpu.VMEM((SIDES * 64, RIM), BF16),
            pltpu.VMEM((32 * 8, 128), F32),
            pltpu.VMEM((32, SIDES * 64), BF16),
            pltpu.VMEM((5, 64, 128), F32),
            pltpu.VMEM((64, 128), F32),
            pltpu.VMEM((3, 32, 128), F32),
            pltpu.VMEM((32, 14, 128), F32),
            pltpu.VMEM((32, 14, 128), F32),
            pltpu.VMEM((3, 32, 3, 128), F32),
            pltpu.VMEM((3, 32, 3, 128), F32),
            pltpu.VMEM((4, 1, 128), F32),
            pltpu.VMEM((2, PLANE, 1, 128), F32),
            pltpu.VMEM((2, LINE, 1, 128), F32),
            dma((8,)),
            dma((1,)),
            dma((1,)),
            dma((3,)),
            dma((3,)),
            dma((4,)),
            dma((4,)),
        ],
        compiler_params=pltpu.CompilerParams(
            collective_id=0, has_side_effects=True, vmem_limit_bytes=56 * 1024 * 1024
        ),
    )(*arguments)
    return tuple(outs[48*i:48*i+48].reshape(1, 1, 1, 6, GRAINS) for i in range(2))


def solution(mesh):
    placed = P("gx", "gy", "gz", None, None)
    flat = P("gx", "gy", "gz", None)
    return jax.shard_map(
        shards,
        mesh=mesh,
        in_specs=(placed, placed, P(), flat, flat, flat, placed, placed),
        out_specs=(placed, placed),
        check_vma=False,
    )
```

```python
import functools

import jax
import jax.numpy as jnp
from jax import lax
from jax.experimental import pallas as pl
from jax.experimental.pallas import tpu as pltpu
from jax.sharding import PartitionSpec as P

F32 = jnp.float32
BF16 = jnp.bfloat16
MESH = pl.DeviceIdType.MESH
GRAINS = 1024
RIM = 256
NEAR = 2240
TYPES = 4
SIDES = 26
LOCAL_ROWS = 18
NX, NY, NZ = 4, 8, 16
ZLO = 4
PLANE = 32
LINE = 16


def offset_of(side):
    whole = side + (1 if side >= 13 else 0)
    return (whole // 9 - 1, whole // 3 % 3 - 1, whole % 3 - 1)


def cross(w, n):
    return [
        w[1] * n[2] - w[2] * n[1],
        w[2] * n[0] - w[0] * n[2],
        w[0] * n[1] - w[1] * n[0],
    ]


def response(a, b, n, ra, rb, coeff, both):
    shear, normal_less, roll, twist_less = coeff
    arm = [rb * b[3 + c] + ra * a[3 + c] for c in range(3)]
    turn = cross(arm, n)
    delta = [b[c] - a[c] - turn[c] for c in range(3)]
    along = normal_less * (n[0] * delta[0] + n[1] * delta[1] + n[2] * delta[2])
    force = [shear * delta[c] + along * n[c] for c in range(3)]
    theta = [b[3 + c] - a[3 + c] for c in range(3)]
    twist = twist_less * (n[0] * theta[0] + n[1] * theta[1] + n[2] * theta[2])
    moment = [roll * theta[c] + twist * n[c] for c in range(3)]
    lever = cross(n, force)
    first = force + [ra * lever[c] + moment[c] for c in range(3)]
    if not both:
        work = [force[c] * delta[c] + moment[c] * theta[c] for c in range(3)]
        return first, work[0] + work[1] + work[2]
    second = [-f for f in force] + [rb * lever[c] - moment[c] for c in range(3)]
    return first, second


def lanes(x, index):
    return jnp.take_along_axis(x, index, axis=1, mode="promise_in_bounds")


def splat(row):
    return jnp.broadcast_to(row, (8, 128))


def kernel(
    rhs_in, diag_in, stiff_in, own_in, slot_in, type_in, normal_in, radii_in,
    x_ref,
    rhs_ref, diag_ref, stiff_ref, own_ref, slot_ref, type_ref, normal_ref, radii_ref,
    dense, idx_a, idx_b, geo, one_hot, t_local, lhs_local,
    rim_idx, rim_far, rim_out, rim_geo, rim_hot, t_rim, lhs_rim, field, diag, mine,
    send_q, recv_q, send_v, recv_v, row_buf, plane_buf, line_buf,
    out_sem, q_recv, v_recv, s_recv,
):
    loads = []
    for j, (source, target) in enumerate((
        (rhs_in, rhs_ref), (own_in, own_ref), (slot_in, slot_ref), (type_in, type_ref),
        (normal_in, normal_ref), (radii_in.at[0, 0, 0], radii_ref), (stiff_in, stiff_ref),
        (diag_in, diag_ref),
    )):
        load = pltpu.make_async_copy(source, target, out_sem.at[j])
        load.start()
        loads.append(load)
    gx, gy, gz = lax.axis_index("gx"), lax.axis_index("gy"), lax.axis_index("gz")
    wide, low = gz // ZLO, gz % ZLO

    def distance(side):
        dx, dy, dz = offset_of(side)
        return (dx == 0, dx * dz >= 0, -abs(dz), -abs(dy))

    farthest_first = sorted(range(SIDES), key=distance)
    near = []
    for side in range(SIDES):
        dx, dy, dz = offset_of(side)
        near.append(((gx + (dx + NX)) % NX, (gy + (dy + NY)) % NY, (gz + (dz + NZ)) % NZ))
    plane = []
    for j in range(1, PLANE):
        dy, dw = j // ZLO, j % ZLO
        plane.append((gx, (gy + dy) % NY, ((wide + dw) % ZLO) * ZLO + low))
    line = []
    for j in range(1, LINE):
        dx, dl = j // ZLO, j % ZLO
        line.append(((gx + dx) % NX, gy, wide * ZLO + (low + dl) % ZLO))
    plane_rank = gy * ZLO + wide
    line_rank = gx * ZLO + low

    lane = lax.broadcasted_iota(jnp.int32, (8, 128), 1)
    row = lax.broadcasted_iota(jnp.int32, (8, 128), 0)

    barrier = pltpu.get_barrier_semaphore()
    for where in [near[side] for side in farthest_first] + line + plane:
        pl.semaphore_signal(barrier, inc=1, device_id=where, device_id_type=MESH)

    recv_q[0:2] = jnp.zeros((2, 14, 128), F32)
    recv_q[28:32] = jnp.zeros((4, 14, 128), F32)
    for e in range(3):
        recv_v[e, 0:2] = jnp.zeros((2, 3, 128), F32)
        recv_v[e, 28:32] = jnp.zeros((4, 3, 128), F32)

    for load in loads:
        load.wait()

    dense[0] = own_ref[...].astype(F32)
    dense[1] = slot_ref[...].astype(F32)
    dense[2] = type_ref[...].astype(F32)
    for c in range(3):
        dense[3 + c] = normal_ref[24 * c : 24 * c + 24, :]
    for c in range(2):
        for i in range(24):
            dense[6 + c, i : i + 1, :] = radii_ref[c : c + 1, 128 * i : 128 * (i + 1)]

    stiffness = [
        [jnp.broadcast_to(stiff_ref[q : q + 1, t : t + 1], (8, 128)) for t in range(TYPES)]
        for q in range(4)
    ]

    def coefficients(kind, valid):
        out = []
        for q in range(4):
            total = jnp.zeros_like(kind)
            for t in range(TYPES):
                total = jnp.where(kind == float(t), stiffness[q][t], total)
            out.append(jnp.where(valid, total, 0.0))
        return [out[1], out[0] - out[1], out[2], out[3] - out[2]]

    def segments(q, v):
        low_row = dense[q, 17 + 2 * v : 18 + 2 * v, :]
        nxt = min(18 + 2 * v, 23)
        high_row = dense[q, nxt : nxt + 1, :]
        base = jnp.where(row < 4, splat(low_row), splat(high_row))
        return lanes(base, (lane % 32) + 32 * (row % 4))

    def quarter(parts):
        out = parts[3]
        for p in (2, 1, 0):
            out = jnp.where(lane < 32 * (p + 1), parts[p], out)
        return out

    kept = []
    for v in range(4):
        seg = [segments(q, v) for q in range(8)]
        side = (row + (8 * v - 2)).astype(F32)
        slot_rim = seg[1] - (GRAINS + RIM * side)
        rows = slice(8 * v, 8 * v + 8)
        send_q[rows, 12, :] = quarter([slot_rim, seg[2], seg[6], seg[7]])
        send_q[rows, 13, :] = quarter([seg[3], seg[4], seg[5], seg[0]])
        seg[1] = slot_rim
        kept.append(seg)
    for v in range(4):
        for q in range(8):
            rim_geo[q, 8 * v : 8 * v + 8, :] = kept[v][q]
    rim = jnp.concatenate([rhs_ref[8 * c : 8 * c + 2, :] for c in range(6)], axis=0)
    for side in range(SIDES):
        send_q[side + 2, 0:12, :] = rim

    pl.semaphore_wait(barrier, SIDES + PLANE - 1 + LINE - 1)

    def exchange(source, target, send_sem, recv_sem):
        for side in farthest_first:
            pltpu.make_async_remote_copy(
                src_ref=source.at[side + 2],
                dst_ref=target.at[27 - side],
                send_sem=send_sem,
                recv_sem=recv_sem,
                device_id=near[side],
                device_id_type=MESH,
            ).start()
        return pltpu.make_async_remote_copy(
            src_ref=source.at[2:28],
            dst_ref=target.at[2:28],
            send_sem=send_sem,
            recv_sem=recv_sem,
            device_id=near[0],
            device_id_type=MESH,
        )

    arriving = exchange(send_q, recv_q, out_sem.at[0], q_recv.at[0])

    for v in range(3):
        rows = slice(8 * v, 8 * v + 8)
        number = (row + 8 * v) * 128 + lane
        inside = number < NEAR
        own = dense[0, rows, :]
        slot = jnp.where(inside, dense[1, rows, :], 0.0)
        idx_a[rows, :] = own.astype(jnp.int32)
        idx_b[rows, :] = slot.astype(jnp.int32)
        dense[1, rows, :] = slot
        coeff = coefficients(dense[2, rows, :], inside)
        for q in range(4):
            geo[q, rows, :] = coeff[q]

    column = lax.broadcasted_iota(jnp.int32, (128, 128), 1).astype(F32)
    pad = jnp.zeros((128 - 24, 128), F32)
    for which in range(2):
        turned = jnp.transpose(jnp.concatenate([dense[which], pad], axis=0))
        for j in range(LOCAL_ROWS):
            spread = jnp.broadcast_to(turned[:, j : j + 1], (128, 128))
            at = (which * LOCAL_ROWS + j) * 128
            for g in range(8):
                hit = jnp.where(spread == column + float(128 * g), 1.0, 0.0)
                one_hot[at : at + 128, 128 * g : 128 * (g + 1)] = hit.astype(BF16)

    def rim_rows(turned, first_row, at):
        for i in range(SIDES):
            spread_idx = jnp.broadcast_to(turned[first_row : first_row + 32, i + 2 : i + 3], (32, 128))
            start = 64 * i + at
            for g in range(2):
                hit = jnp.where(spread_idx == column[0:32] + float(128 * g), 1.0, 0.0)
                rim_hot[start : start + 32, 128 * g : 128 * (g + 1)] = hit.astype(BF16)

    rim_pad = jnp.zeros((96, 128), F32)
    rim_rows(jnp.transpose(jnp.concatenate([rim_geo[0], rim_pad], axis=0)), 0, 32)

    t_local[...] = jnp.zeros_like(t_local)
    t_rim[...] = jnp.zeros_like(t_rim)
    lhs_local[...] = jnp.zeros_like(lhs_local)
    lhs_rim[...] = jnp.zeros_like(lhs_rim)

    field[0, 0:48, :] = rhs_ref[...]
    field[0, 48:64, :] = jnp.zeros((16, 128), F32)
    diag[0:48, :] = diag_ref[...]
    diag[48:64, :] = jnp.zeros((16, 128), F32)

    def split_rows(whole, target, at):
        high = whole.astype(BF16).astype(F32)
        rest = whole - high
        mid = rest.astype(BF16).astype(F32)
        low_part = rest - mid
        cut = slice(128 * at, 128 * (at + 1))
        target[0:16, cut] = jnp.concatenate([high, mid], axis=0).astype(BF16)
        target[16:32, cut] = jnp.concatenate([low_part, jnp.zeros_like(low_part)], axis=0).astype(BF16)

    def scatter(lhs, hot):
        out = jnp.dot(lhs[...], hot[...], preferred_element_type=F32)
        return out[0:8] + out[8:16] + out[16:24]

    def local_forces(k):
        for v in range(3):
            rows = slice(8 * v, 8 * v + 8)
            ends = []
            for index_ref in (idx_a, idx_b):
                index = index_ref[rows, :]
                fine, coarse = index % 128, index // 128
                hits = [coarse == t for t in range(1, 8)]
                got = []
                for c in range(6):
                    total = lanes(splat(field[k, 8 * c : 8 * c + 1, :]), fine)
                    for t in range(1, 8):
                        table = splat(field[k, 8 * c + t : 8 * c + t + 1, :])
                        total = jnp.where(hits[t - 1], lanes(table, fine), total)
                    got.append(total)
                ends.append(got)
            first, second = response(
                ends[0], ends[1],
                [dense[3 + c, rows, :] for c in range(3)],
                dense[6, rows, :], dense[7, rows, :],
                [geo[q, rows, :] for q in range(4)], True,
            )
            for c in range(6):
                t_local[pl.ds(64 * v + c, 8, stride=8), :] = first[c]
                t_local[pl.ds(192 + 64 * v + c, 8, stride=8), :] = second[c]
        for which in range(2):
            for j in range(LOCAL_ROWS):
                start = 8 * (which * 24 + j)
                split_rows(t_local[start : start + 8, :], lhs_local, which * LOCAL_ROWS + j)
        return scatter(lhs_local, one_hot)

    def rim_values(k, index_ref, v):
        index = index_ref[8 * v : 8 * v + 8, :]
        fine, upper = index % 128, index >= 128
        out = []
        for pair in range(3):
            got = []
            for c in (2 * pair, 2 * pair + 1):
                halves = [lanes(splat(field[k, 8 * c + t : 8 * c + t + 1, :]), fine) for t in range(2)]
                got.append(jnp.where(upper, halves[1], halves[0]))
            out.append(jnp.where(lane < 64, got[0], got[1]))
        return out

    def own_values(k):
        for v in range(4):
            got = rim_values(k, rim_idx, v)
            for pair in range(3):
                mine[pair, 8 * v : 8 * v + 8, :] = got[pair]

    def send_values(k):
        for v in range(4):
            got = rim_values(k, rim_out, v)
            for pair in range(3):
                send_v[k - 1, 8 * v : 8 * v + 8, pair, :] = got[pair]
        out = exchange(send_v.at[k - 1], recv_v.at[k - 1], out_sem.at[k], v_recv.at[k - 1])
        own_values(k)
        return out

    def rim_contacts(k):
        work = jnp.zeros((8, 128), F32)
        for v in range(4):
            rows = slice(8 * v, 8 * v + 8)
            a, b = [], []
            for pair in range(3):
                own = mine[pair, rows, :]
                a += [own, pltpu.roll(own, 64, 1)]
                if k > 0:
                    got = recv_v[k - 1, rows, pair, :]
                    b += [got, pltpu.roll(got, 64, 1)]
                else:
                    far = rim_far[rows, :]
                    for c in (2 * pair, 2 * pair + 1):
                        halves = [lanes(recv_q[rows, 2 * c + t, :], far % 128) for t in range(2)]
                        b.append(jnp.where(far >= 128, halves[1], halves[0]))
            first, done = response(
                a, b,
                [rim_geo[c, rows, :] for c in range(3)],
                rim_geo[3, rows, :], rim_geo[4, rows, :],
                [rim_geo[5 + q, rows, :] for q in range(4)], False,
            )
            for c in range(6):
                t_rim[pl.ds(64 * v + c, 8, stride=8), :] = first[c]
            work = work + done
        return jnp.sum(jnp.where(lane >= 32, work, 0.0), keepdims=True)

    def rim_forces():
        for i in range(SIDES // 2):
            start = 16 * (i + 1)
            even, odd = t_rim[start : start + 8, :], t_rim[start + 8 : start + 16, :]
            split_rows(jnp.where(lane < 64, even, pltpu.roll(odd, 64, 1)), lhs_rim, i)
        return scatter(lhs_rim, rim_hot)

    sums = []

    def total_of(x):
        folded = x[0:8]
        for t in range(1, 6):
            folded = folded + x[8 * t : 8 * t + 8]
        return jnp.sum(folded, keepdims=True)

    lane_row = lane[0:1]

    def pack(values):
        out = jnp.zeros((1, 128), F32)
        for j, value in enumerate(values):
            out = jnp.where(lane_row == j, value, out)
        return out

    def spread(stage, where, buffer, rank, value):
        row_buf[stage] = value
        buffer[rank] = value
        for device in where:
            pltpu.make_async_remote_copy(
                src_ref=row_buf.at[stage],
                dst_ref=buffer.at[rank],
                send_sem=out_sem.at[4 + stage],
                recv_sem=s_recv.at[stage],
                device_id=device,
                device_id_type=MESH,
            ).start()
        count = len(where)
        return pltpu.make_async_remote_copy(
            src_ref=buffer.at[0:count],
            dst_ref=buffer.at[0:count],
            send_sem=out_sem.at[4 + stage],
            recv_sem=s_recv.at[stage],
            device_id=where[0],
            device_id_type=MESH,
        )

    def gather_sum(arriving, buffer, count):
        arriving.wait_recv()
        level = [buffer[j] for j in range(count)]
        while len(level) > 1:
            level = [level[j] + level[j + 1] for j in range(0, len(level), 2)]
        return level[0]

    def lane_of(values, j):
        return jnp.sum(jnp.where(lane_row == j, values, 0.0), keepdims=True)

    def meet():
        for v in range(4):
            rows = slice(8 * v, 8 * v + 8)
            seg = [rim_geo[q, rows, :] for q in range(8)]
            got = [recv_q[rows, 12 + h, :] for h in range(2)]

            def theirs(h, p):
                return lanes(got[h], lane % 32 + 32 * p)

            ours = lane % 64 >= 32
            valid = (lane < 64) & (row + 8 * v >= 2) & (row + 8 * v < 28)
            index = jnp.where(ours, seg[0], theirs(0, 0))
            kind = jnp.where(ours, seg[2], theirs(0, 1))
            rim_idx[rows, :] = index.astype(jnp.int32)
            flipped = jnp.where(ours, theirs(0, 0), seg[0])
            rim_out[rows, :] = flipped.astype(jnp.int32)
            rim_far[rows, :] = jnp.where(ours, seg[1], theirs(1, 3)).astype(jnp.int32)
            for c in range(3):
                rim_geo[c, rows, :] = jnp.where(ours, seg[3 + c], -theirs(1, c))
            rim_geo[3, rows, :] = jnp.where(ours, seg[6], theirs(0, 3))
            rim_geo[4, rows, :] = jnp.where(ours, seg[7], theirs(0, 2))
            coeff = coefficients(kind, valid)
            for q in range(4):
                rim_geo[5 + q, rows, :] = coeff[q]
        own_values(0)
        turned = jnp.transpose(jnp.concatenate([rim_idx[...].astype(F32), rim_pad], axis=0))
        rim_rows(turned, 0, 0)

    sent = [arriving]

    def tile(ref, t):
        return ref[pl.ds(t, 8, stride=8), :]

    def product(k, t, forces):
        return tile(diag, t) * tile(field.at[k], t) - forces

    def apply(k, arriving, finish, between=None):
        whole = local_forces(k)
        if between is not None:
            between()
        for t in range(2, 8):
            field[k + 1, pl.ds(t, 8, stride=8), :] = finish(product(k, t, whole[:, 128 * t : 128 * (t + 1)]), t)
        start = [product(k, t, whole[:, 128 * t : 128 * (t + 1)]) for t in range(2)]
        arriving.wait_recv()
        if k == 0:
            meet()
        rim_contacts(k)
        rim = rim_forces()
        for t in range(2):
            value = start[t] - rim[:, 128 * t : 128 * (t + 1)]
            field[k + 1, pl.ds(t, 8, stride=8), :] = finish(value, t)
        out = send_values(k + 1)
        sent.append(out)
        return out

    def plain(value, t):
        return value

    def dense_of(k):
        return field[k, 0:48, :]

    w0 = dense_of(0)
    arriving = apply(0, arriving, plain)
    w1 = dense_of(1)
    first_sums = pack([total_of(w0 * w0), total_of(w0 * w1), total_of(w1 * w1)])
    early = spread(0, plane, plane_buf.at[0], plane_rank, first_sums)
    sent.append(early)
    held = {}

    def onward():
        held["line"] = spread(1, line, line_buf.at[0], line_rank, gather_sum(early, plane_buf.at[0], PLANE))
        sent.append(held["line"])

    arriving = apply(1, arriving, plain, onward)

    def settle():
        total = gather_sum(held["line"], line_buf.at[0], LINE)
        m0, m1, m2 = lane_of(total, 0), lane_of(total, 1), lane_of(total, 2)
        held["inv"] = jnp.sqrt(m0 / m2)
        held["shift"] = m1 / m0 * held["inv"]

    def centred(value, t):
        inv, shift = held["inv"], held["shift"]
        inv2 = inv * inv
        b, p, q = [tile(field.at[j], t) for j in range(3)]
        p, q = p * inv, q * inv2
        return value * (inv2 * inv) - shift * (3.0 * q - shift * (3.0 * p - shift * b))

    arriving = apply(2, arriving, centred, settle)
    inv, shift = held["inv"], held["shift"]
    u0, u3 = w0, dense_of(3)
    p, q = w1 * inv, dense_of(2) * (inv * inv)
    u1 = p - shift * u0
    u2 = q - shift * (2.0 * p - shift * u0)
    basis = [u0, u1, u2, u3]
    pairs = [(0, 0), (0, 1), (1, 1), (1, 2), (2, 2), (2, 3), (3, 3)]
    known = [total_of(basis[i] * basis[j]) for i, j in pairs]
    whole = local_forces(3)
    near_work = jnp.zeros((8, 128), F32)
    for t in range(8):
        value = product(3, t, whole[:, 128 * t : 128 * (t + 1)])
        field[4, pl.ds(t, 8, stride=8), :] = value
        near_work = near_work + value * tile(field.at[3], t)
    near_work = inv * jnp.sum(near_work, keepdims=True) - shift * known[6]
    arriving.wait_recv()
    last = near_work + inv * rim_contacts(3)
    late = spread(2, plane, plane_buf.at[1], plane_rank, pack(known + [last]))
    rim = rim_forces()
    for t in range(2):
        value = tile(field.at[4], t) - rim[:, 128 * t : 128 * (t + 1)]
        field[4, pl.ds(t, 8, stride=8), :] = value
    u4 = dense_of(4) * inv - shift * u3
    for done in sent:
        done.wait_send()
    sums = gather_sum(late, plane_buf.at[1], PLANE)
    late.wait_send()
    late = spread(3, line, line_buf.at[1], line_rank, sums)
    sums = gather_sum(late, line_buf.at[1], LINE)
    late.wait_send()
    mu = [lane_of(sums, j) for j in range(8)]

    scale = 1.0 / inv

    def inner(p, q):
        by_degree = {}
        for i, x in enumerate(p):
            for j, y in enumerate(q):
                term = x * y
                by_degree[i + j] = by_degree[i + j] + term if i + j in by_degree else term
        out = None
        for degree, term in by_degree.items():
            term = term * mu[degree]
            out = term if out is None else out + term
        return out

    one = jnp.ones((1, 1), F32)
    res, direction, answer = [one], [one], []
    norm = mu[0]
    for step in range(4):
        image = [shift * direction[0]]
        for i in range(1, len(direction)):
            image.append(direction[i - 1] + shift * direction[i])
        image.append(direction[-1])
        image = [scale * value for value in image]
        alpha = norm / inner(direction, image)
        answer = [
            alpha * direction[i] + (answer[i] if i < len(answer) else 0.0)
            for i in range(len(direction))
        ]
        res = [
            (res[i] if i < len(res) else 0.0) - alpha * image[i]
            for i in range(len(image))
        ]
        if step < 3:
            fresh = inner(res, res)
            ratio = fresh / norm
            direction = [
                res[i] + (ratio * direction[i] if i < len(direction) else 0.0)
                for i in range(len(res))
            ]
            norm = fresh
    basis.append(u4)
    x = answer[0] * basis[0]
    for i in range(1, 4):
        x = x + answer[i] * basis[i]
    r = res[0] * basis[0]
    for i in range(1, 5):
        r = r + res[i] * basis[i]
    x_ref[0:48] = x
    x_ref[48:96] = r


def shards(*arguments):
    arguments = [
        x if x.ndim == 2 or x.shape[3] == 2 else x.reshape(x.size // 128, 128) for x in arguments
    ]
    vmem = pl.BlockSpec(memory_space=pltpu.VMEM)
    hbm = pl.BlockSpec(memory_space=pltpu.HBM)
    out = jax.ShapeDtypeStruct((48, 128), F32)
    dma = pltpu.SemaphoreType.DMA
    outs = pl.pallas_call(
        kernel,
        out_shape=pltpu.VMEM((96, 128), F32),
        in_specs=[hbm] * 8,
        out_specs=vmem,
        scratch_shapes=[
            pltpu.VMEM((48, 128), F32),
            pltpu.VMEM((48, 128), F32),
            pltpu.VMEM((4, 4), F32),
            pltpu.VMEM((24, 128), jnp.int32),
            pltpu.VMEM((24, 128), jnp.int32),
            pltpu.VMEM((24, 128), jnp.int32),
            pltpu.VMEM((72, 128), F32),
            pltpu.VMEM((2, 3072), F32),
            pltpu.VMEM((8, 24, 128), F32),
            pltpu.VMEM((24, 128), jnp.int32),
            pltpu.VMEM((24, 128), jnp.int32),
            pltpu.VMEM((4, 24, 128), F32),
            pltpu.VMEM((2 * LOCAL_ROWS * 128, GRAINS), BF16),
            pltpu.VMEM((2 * 24 * 8, 128), F32),
            pltpu.VMEM((32, 2 * LOCAL_ROWS * 128), BF16),
            pltpu.VMEM((32, 128), jnp.int32),
            pltpu.VMEM((32, 128), jnp.int32),
            pltpu.VMEM((32, 128), jnp.int32),
            pltpu.VMEM((9, 32, 128), F32),
            pltpu.VMEM((SIDES * 64, RIM), BF16),
            pltpu.VMEM((32 * 8, 128), F32),
            pltpu.VMEM((32, SIDES * 64), BF16),
            pltpu.VMEM((5, 64, 128), F32),
            pltpu.VMEM((64, 128), F32),
            pltpu.VMEM((3, 32, 128), F32),
            pltpu.VMEM((32, 14, 128), F32),
            pltpu.VMEM((32, 14, 128), F32),
            pltpu.VMEM((3, 32, 3, 128), F32),
            pltpu.VMEM((3, 32, 3, 128), F32),
            pltpu.VMEM((4, 1, 128), F32),
            pltpu.VMEM((2, PLANE, 1, 128), F32),
            pltpu.VMEM((2, LINE, 1, 128), F32),
            dma((8,)),
            dma((1,)),
            dma((3,)),
            dma((4,)),
        ],
        compiler_params=pltpu.CompilerParams(
            collective_id=0, has_side_effects=True, vmem_limit_bytes=56 * 1024 * 1024
        ),
    )(*arguments)
    return tuple(outs[48*i:48*i+48].reshape(1, 1, 1, 6, GRAINS) for i in range(2))


def solution(mesh):
    placed = P("gx", "gy", "gz", None, None)
    flat = P("gx", "gy", "gz", None)
    return jax.shard_map(
        shards,
        mesh=mesh,
        in_specs=(placed, placed, P(), flat, flat, flat, placed, placed),
        out_specs=(placed, placed),
        check_vma=False,
    )
```
